16 devices in a mesh: dp: 4 (over z, y), tp: 4 (over x, core).
Axes of the slice: x: 2, y: 2, z: 2, core: 2. Of those that a mesh axis runs over, the one named last changes fastest.
Arguments:
- x_in: bfloat16 [32, 1024, 768], P('dp', 'tp'), parts along dimension 0
- cond_vec: bfloat16 [32, 768], P('dp'), parts along dimension 0
- rope_cos: float32 [1024, 32], P('tp')
- rope_sin: float32 [1024, 32], P('tp')
- w_mod: bfloat16 [2, 768, 2304], replicated
- b_mod: bfloat16 [2, 2304], replicated
- w_in: bfloat16 [2, 768, 12, 448], P(None, None, 'tp')
- b_in: bfloat16 [2, 12, 448], P(None, 'tp')
- q_scale: bfloat16 [2, 64], replicated
- k_scale: bfloat16 [2, 64], replicated
- w_out: bfloat16 [2, 12, 320, 768], P(None, 'tp')
- b_out: bfloat16 [2, 768], replicated
- d_out: bfloat16 [32, 1024, 768], P('dp', 'tp'), parts along dimension 0
Outputs:
- output 1: bfloat16 [32, 1024, 768], P('dp', 'tp'), parts along dimension 0
- output 2: bfloat16 [32, 1024, 768], P('dp', 'tp'), parts along dimension 0
- output 3: float32 [8, 768, 2304], P('dp'), parts along dimension 0
- output 4: float32 [8, 2304], P('dp'), parts along dimension 0
- output 5: bfloat16 [8, 768, 12, 448], P('dp', None, 'tp'), parts along dimension 0
- output 6: float32 [8, 12, 448], P('dp', 'tp'), parts along dimension 0
- output 7: float32 [8, 64], P('dp'), parts along dimension 0
- output 8: float32 [8, 64], P('dp'), parts along dimension 0
- output 9: bfloat16 [8, 12, 320, 768], P('dp', 'tp'), parts along dimension 0
- output 10: float32 [8, 768], P('dp'), parts along dimension 0
There are 4 independent parts. The reference program is written for one: setup_inputs(seed, part) draws one part's arguments, and reference() takes and returns one part's arrays. A program takes and returns all parts, laid end to end along the dimension named above; an argument that names none is the same for every part.
All inputs are finite; a program needn't handle non-finite values.
Results may differ from the reference program's by a relative error of at most 0.02.
Values are sent between devices in bfloat16 or wider.
A program may use at most 1 GiB of HBM per device.

```python
import jax
import jax.numpy as jnp
from jax import lax

MODEL_DIM = 768
NUM_HEADS = 12
HEAD_DIM = 64
MLP_DIM = 3072
SEQ_LEN = 1024
BATCH_SIZE = 8
NUM_BLOCKS = 2

GROUP_MLP = MLP_DIM // NUM_HEADS
GROUP_COLS = 3 * HEAD_DIM + GROUP_MLP
GROUP_ROWS = HEAD_DIM + GROUP_MLP
TEXT_LEN = SEQ_LEN // 4
HALF_DIM = HEAD_DIM // 2
NORM_EPS = 1e-6


def rope_tables(table_key):
    key_w, key_r, key_c = jax.random.split(table_key, 3)
    grid_width = jax.random.randint(key_w, (), 8, 65)
    row_off = jax.random.randint(key_r, (), 0, 32)
    col_off = jax.random.randint(key_c, (), 0, 32)
    token_idx = jnp.arange(SEQ_LEN) - TEXT_LEN
    is_image = token_idx >= 0
    safe_idx = jnp.maximum(token_idx, 0)
    row_pos = jnp.where(is_image, safe_idx // grid_width + row_off, 0).astype(jnp.float32)
    col_pos = jnp.where(is_image, safe_idx % grid_width + col_off, 0).astype(jnp.float32)
    n_zero = HALF_DIM // 8
    n_row = (HALF_DIM - n_zero) // 2
    n_col = HALF_DIM - n_zero - n_row
    freq_row = 10000.0 ** (-jnp.arange(n_row, dtype=jnp.float32) / n_row)
    freq_col = 10000.0 ** (-jnp.arange(n_col, dtype=jnp.float32) / n_col)
    angles = jnp.concatenate([jnp.zeros((SEQ_LEN, n_zero), jnp.float32), row_pos[:, None] * freq_row[None, :], col_pos[:, None] * freq_col[None, :]], axis=1)
    return jnp.cos(angles), jnp.sin(angles)


def setup_inputs(seed: int = 0, part: int = 0) -> dict:
    base_key = jax.random.key(seed)
    shared_keys = jax.random.split(base_key, 12)
    own_keys = jax.random.split(jax.random.fold_in(base_key, part), 4)
    is_text = (jnp.arange(SEQ_LEN) < TEXT_LEN)[None, :, None]
    x_raw = jax.random.normal(own_keys[0], (BATCH_SIZE, SEQ_LEN, MODEL_DIM), jnp.float32)
    text_shift = 0.8 * jax.random.normal(own_keys[1], (MODEL_DIM,), jnp.float32)
    x_in = jnp.where(is_text, 0.6 * x_raw + text_shift, x_raw)
    cond_vec = jax.random.normal(own_keys[2], (BATCH_SIZE, MODEL_DIM), jnp.float32)
    d_out = jax.random.normal(own_keys[3], (BATCH_SIZE, SEQ_LEN, MODEL_DIM), jnp.float32)
    rope_cos, rope_sin = rope_tables(shared_keys[0])
    w_mod = jax.random.normal(shared_keys[1], (NUM_BLOCKS, MODEL_DIM, 3 * MODEL_DIM), jnp.float32) * MODEL_DIM ** -0.5
    b_mod = 0.5 * jax.random.normal(shared_keys[2], (NUM_BLOCKS, 3 * MODEL_DIM), jnp.float32)
    w_in = jax.random.normal(shared_keys[3], (NUM_BLOCKS, MODEL_DIM, NUM_HEADS, GROUP_COLS), jnp.float32) * MODEL_DIM ** -0.5
    b_in = 0.3 * jax.random.normal(shared_keys[4], (NUM_BLOCKS, NUM_HEADS, GROUP_COLS), jnp.float32)
    q_scale = 1.5 + 0.4 * jax.random.normal(shared_keys[5], (NUM_BLOCKS, HEAD_DIM), jnp.float32)
    k_scale = 1.5 + 0.4 * jax.random.normal(shared_keys[6], (NUM_BLOCKS, HEAD_DIM), jnp.float32)
    w_out = jax.random.normal(shared_keys[7], (NUM_BLOCKS, NUM_HEADS, GROUP_ROWS, MODEL_DIM), jnp.float32) * (MODEL_DIM + MLP_DIM) ** -0.5
    b_out = 0.3 * jax.random.normal(shared_keys[8], (NUM_BLOCKS, MODEL_DIM), jnp.float32)
    return {"x_in": x_in.astype(jnp.bfloat16), "cond_vec": cond_vec.astype(jnp.bfloat16), "rope_cos": rope_cos, "rope_sin": rope_sin, "w_mod": w_mod.astype(jnp.bfloat16), "b_mod": b_mod.astype(jnp.bfloat16), "w_in": w_in.astype(jnp.bfloat16), "b_in": b_in.astype(jnp.bfloat16), "q_scale": q_scale.astype(jnp.bfloat16), "k_scale": k_scale.astype(jnp.bfloat16), "w_out": w_out.astype(jnp.bfloat16), "b_out": b_out.astype(jnp.bfloat16), "d_out": d_out.astype(jnp.bfloat16)}


def to_bf16(tensor):
    return tensor.astype(jnp.bfloat16).astype(jnp.float32)


def rms_norm(tensor):
    return tensor * lax.rsqrt(jnp.mean(tensor * tensor, axis=-1, keepdims=True) + NORM_EPS)


def layer_norm(tensor):
    row_mean = jnp.mean(tensor, axis=-1, keepdims=True)
    centered = tensor - row_mean
    row_var = jnp.mean(centered * centered, axis=-1, keepdims=True)
    return centered * lax.rsqrt(row_var + NORM_EPS)


def apply_rope(tensor, rope_cos, rope_sin):
    pair_view = tensor.reshape(tensor.shape[:-1] + (tensor.shape[-1] // 2, 2))
    even_part = pair_view[..., 0]
    odd_part = pair_view[..., 1]
    cos_wide = rope_cos[None, :, None, :]
    sin_wide = rope_sin[None, :, None, :]
    rotated = jnp.stack([even_part * cos_wide - odd_part * sin_wide, even_part * sin_wide + odd_part * cos_wide], axis=-1)
    return rotated.reshape(tensor.shape)


def head_attention(operands):
    q_head, k_head, v_head = operands
    scores = jnp.einsum("bqe,bke->bqk", q_head, k_head) * (HEAD_DIM ** -0.5)
    attn_probs = jax.nn.softmax(scores, axis=-1)
    return to_bf16(jnp.einsum("bqk,bke->bqe", to_bf16(attn_probs), v_head))


def block_forward(x_f32, silu_vec, rope_cos, rope_sin, layer_params):
    w_mod, b_mod, w_in, b_in, q_scale, k_scale, w_out, b_out = layer_params
    mod_vec = jnp.dot(silu_vec, w_mod, preferred_element_type=jnp.float32) + b_mod
    mod_shift, mod_scale, mod_gate = jnp.split(mod_vec, 3, axis=-1)
    normed = to_bf16(layer_norm(x_f32) * (1.0 + mod_scale[:, None, :]) + mod_shift[:, None, :])
    projected = jnp.einsum("bsd,dhc->bshc", normed, w_in) + b_in
    q_rot = to_bf16(apply_rope(rms_norm(projected[..., :HEAD_DIM]) * q_scale, rope_cos, rope_sin))
    k_rot = to_bf16(apply_rope(rms_norm(projected[..., HEAD_DIM:2 * HEAD_DIM]) * k_scale, rope_cos, rope_sin))
    v_part = to_bf16(projected[..., 2 * HEAD_DIM:3 * HEAD_DIM])
    mlp_act = to_bf16(jax.nn.gelu(projected[..., 3 * HEAD_DIM:], approximate=True))
    per_head = lax.map(jax.checkpoint(head_attention), (jnp.moveaxis(q_rot, 2, 0), jnp.moveaxis(k_rot, 2, 0), jnp.moveaxis(v_part, 2, 0)))
    attn_out = jnp.moveaxis(per_head, 0, 2)
    joined = jnp.concatenate([attn_out, mlp_act], axis=-1)
    mixed_out = jnp.einsum("bshc,hcd->bsd", joined, w_out)
    return to_bf16(x_f32 + mod_gate[:, None, :] * (mixed_out + b_out))


def reference(x_in, cond_vec, rope_cos, rope_sin, w_mod, b_mod, w_in, b_in, q_scale, k_scale, w_out, b_out, d_out):
    silu_vec = to_bf16(jax.nn.silu(cond_vec.astype(jnp.float32)))
    weights = tuple(weight.astype(jnp.float32) for weight in (w_mod, b_mod, w_in, b_in, q_scale, k_scale, w_out, b_out))

    def stack_forward(x_f32, all_params):
        def layer_step(state_in, layer_params):
            return block_forward(state_in, silu_vec, rope_cos, rope_sin, layer_params), None
        final_state, unused = lax.scan(layer_step, x_f32, all_params)
        return final_state

    out_f32, pullback = jax.vjp(stack_forward, x_in.astype(jnp.float32), weights)
    grad_x, grad_w = pullback(d_out.astype(jnp.float32))
    return (out_f32.astype(jnp.bfloat16), grad_x.astype(jnp.bfloat16), grad_w[0], grad_w[1], grad_w[2].astype(jnp.bfloat16), grad_w[3], grad_w[4], grad_w[5], grad_w[6].astype(jnp.bfloat16), grad_w[7])
```

```python
import functools
import jax
import jax.numpy as jnp
import numpy as np
from jax import lax
from jax.experimental import pallas as pl
from jax.experimental.pallas import tpu as pltpu
from jax.sharding import PartitionSpec as P

NORM_EPS = 1e-6
LOG2E = 1.4426950408889634
GELU_C = 0.7978845608028654
GELU_A = 0.044715
F32 = jnp.float32
BF16 = jnp.bfloat16
CHUNK = 256


def dot_nn(a, b):
    return lax.dot_general(a, b, (((1,), (0,)), ((), ())), preferred_element_type=F32)


def dot_nt(a, b):
    return lax.dot_general(a, b, (((1,), (1,)), ((), ())), preferred_element_type=F32)


def dot_tn(a, b):
    return lax.dot_general(a, b, (((0,), (0,)), ((), ())), preferred_element_type=F32)


def head_weights(w_ref, i):
    return jnp.concatenate([w_ref[d, i, 0] for d in range(w_ref.shape[0])], axis=0)


def norm_rope(raw, scale_col, cos_t, sin_t):
    half = raw.shape[0] // 2
    inv = lax.rsqrt(jnp.mean(raw * raw, axis=0, keepdims=True) + NORM_EPS)
    hat = raw * inv
    scaled = hat * scale_col
    a, b = scaled[:half], scaled[half:]
    rot = jnp.concatenate([a * cos_t - b * sin_t, a * sin_t + b * cos_t], axis=0)
    return hat, inv, rot.astype(BF16)


def norm_rope_bwd(d_rot, hat, inv, scale_col, cos_t, sin_t):
    half = d_rot.shape[0] // 2
    da, db = d_rot[:half], d_rot[half:]
    d_scaled = jnp.concatenate([da * cos_t + db * sin_t, db * cos_t - da * sin_t], axis=0)
    d_scale = jnp.sum(d_scaled * hat, axis=1, keepdims=True)
    d_hat = d_scaled * scale_col
    d_raw = inv * (d_hat - hat * jnp.mean(d_hat * hat, axis=0, keepdims=True))
    return d_raw, d_scale


def fwd_kernel(e, x_ref, mod_ref, w_ref, bin_ref, qs_ref, ks_ref, cos_ref, sin_ref, y_ref, o_ref, lse_ref, h_ref, br_ref, xo_ref, z_sc, h_sc):
    g, b = pl.program_id(0), pl.program_id(1)
    last = pl.num_programs(0) - 1
    cols = bin_ref.shape[2]
    s_len = x_ref.shape[2]

    @pl.when(g == 0)
    def _():
        x = x_ref[0].astype(F32)
        cent = x - jnp.mean(x, axis=0, keepdims=True)
        normed = cent * lax.rsqrt(jnp.mean(cent * cent, axis=0, keepdims=True) + NORM_EPS)
        h = (normed * (1.0 + mod_ref[0, :, 1:2]) + mod_ref[0, :, 0:1]).astype(BF16)
        h_sc[b] = h
        h_ref[0] = h

    h_t = h_sc[b]
    cos_t, sin_t = cos_ref[...], sin_ref[...]
    mul = (e ** -0.5) * LOG2E
    joined, outs = [], []
    for i in range(2):
        w = head_weights(w_ref, i)
        outs.append(w[cols:])
        y = dot_nn(w[:cols], h_t) + bin_ref[i, 0]
        y_ref[0, i, 0] = y
        q_rot = norm_rope(y[:e], qs_ref[...], cos_t, sin_t)[2]
        k_rot = norm_rope(y[e:2 * e], ks_ref[...], cos_t, sin_t)[2]
        v_t = y[2 * e:3 * e].astype(BF16)
        for c in range(s_len // CHUNK):
            span = slice(c * CHUNK, (c + 1) * CHUNK)
            s = dot_tn(k_rot, q_rot[:, span])
            top = jnp.max(s, axis=0, keepdims=True) * mul
            p = jnp.exp2(s * mul - top)
            tot = jnp.sum(p, axis=0, keepdims=True)
            p16 = (p * (1.0 / tot)).astype(BF16)
            o_ref[0, i, 0, :, span] = dot_nn(v_t, p16).astype(BF16)
            lse_ref[0, 0, i:i + 1, span] = top + jnp.log2(tot)
        u = y[3 * e:]
        t = jnp.tanh(GELU_C * (u + GELU_A * u * u * u))
        joined.append(o_ref[0, i, 0])
        joined.append((0.5 * u * (1.0 + t)).astype(BF16))
    z = dot_tn(jnp.concatenate(outs, axis=0), jnp.concatenate(joined, axis=0))

    @pl.when(g == 0)
    def _():
        z_sc[b] = z

    @pl.when(jnp.logical_and(g > 0, g < last))
    def _():
        z_sc[b] += z

    @pl.when(g == last)
    def _():
        branch = z_sc[b] + z + mod_ref[0, :, 3:4]
        br_ref[0] = branch
        xo_ref[0] = (x_ref[0].astype(F32) + mod_ref[0, :, 2:3] * branch).astype(BF16)


def bwd_kernel(e, dbr_ref, h_ref, w_ref, qs_ref, ks_ref, cos_ref, sin_ref, y_ref, o_ref, lse_ref, gw_ref, gb_ref, dqs_ref, dks_ref, dh_ref, dh_sc, acc_sc, dj_sc, dp_sc, jn_sc):
    g, b = pl.program_id(0), pl.program_id(1)
    last = pl.num_programs(0) - 1
    cols = y_ref.shape[3]
    rows = dj_sc.shape[0] // 2
    s_len = dbr_ref.shape[2]
    d_br = dbr_ref[0]
    cos_t, sin_t = cos_ref[...], sin_ref[...]
    scale = e ** -0.5
    mul = scale * LOG2E
    ws = [head_weights(w_ref, i) for i in range(2)]
    for i in range(2):
        dj_sc[i * rows:(i + 1) * rows] = dot_nn(ws[i][cols:], d_br).astype(BF16)

    @pl.when(jnp.logical_and(g == 0, b == 0))
    def _():
        dqs_ref[...] = jnp.zeros_like(dqs_ref)
        dks_ref[...] = jnp.zeros_like(dks_ref)

    @pl.when(b == 0)
    def _():
        gb_ref[...] = jnp.zeros_like(gb_ref)

    for i in range(2):
        base = i * cols
        q_hat, q_inv, q_rot = norm_rope(y_ref[0, i, 0, :e], qs_ref[...], cos_t, sin_t)
        k_hat, k_inv, k_rot = norm_rope(y_ref[0, i, 0, e:2 * e], ks_ref[...], cos_t, sin_t)
        v_t = y_ref[0, i, 0, 2 * e:3 * e].astype(BF16)
        o_t = o_ref[0, i, 0]
        d_o = dj_sc[i * rows:i * rows + e]
        d_sum = jnp.sum(d_o.astype(F32) * o_t.astype(F32), axis=0, keepdims=True)
        d_q, d_k, d_v = [], None, None
        for c in range(s_len // CHUNK):
            span = slice(c * CHUNK, (c + 1) * CHUNK)
            s = dot_tn(k_rot, q_rot[:, span])
            p = jnp.exp2(s * mul - lse_ref[0, 0, i:i + 1, span])
            d_p = dot_tn(v_t, d_o[:, span])
            d_s = (p * (d_p - d_sum[:, span])).astype(BF16)
            d_q.append(dot_nn(k_rot, d_s))
            kc = dot_nt(q_rot[:, span], d_s)
            vc = dot_nt(d_o[:, span], p.astype(BF16))
            d_k = kc if d_k is None else d_k + kc
            d_v = vc if d_v is None else d_v + vc
        d_q = jnp.concatenate(d_q, axis=1) * scale
        d_qraw, d_qs = norm_rope_bwd(d_q, q_hat, q_inv, qs_ref[...], cos_t, sin_t)
        d_kraw, d_ks = norm_rope_bwd(d_k * scale, k_hat, k_inv, ks_ref[...], cos_t, sin_t)
        dqs_ref[...] += d_qs
        dks_ref[...] += d_ks
        u = y_ref[0, i, 0, 3 * e:]
        t = jnp.tanh(GELU_C * (u + GELU_A * u * u * u))
        half = 0.5 * (1.0 + t)
        jn_sc[i * rows:i * rows + e] = o_t
        jn_sc[i * rows + e:(i + 1) * rows] = (u * half).astype(BF16)
        slope = half + 0.5 * u * (1.0 - t * t) * (GELU_C * (1.0 + 3.0 * GELU_A * u * u))
        d_u = dj_sc[i * rows + e:(i + 1) * rows].astype(F32) * slope
        off = 0
        for part in (d_qraw, d_kraw, d_v, d_u):
            n = part.shape[0]
            dp_sc[base + off:base + off + n] = part.astype(BF16)
            gb_ref[i, 0, off:off + n] += jnp.sum(part, axis=1, keepdims=True)
            off += n

    h_t = h_ref[0]
    gwi = dot_nt(dp_sc[...], h_t)
    gwo = dot_nt(jn_sc[...], d_br)
    d_h = dot_tn(jnp.concatenate([ws[0][:cols], ws[1][:cols]], axis=0), dp_sc[...])

    @pl.when(b == 0)
    def _():
        acc_sc[:2 * cols] = gwi
        acc_sc[2 * cols:] = gwo

    @pl.when(b > 0)
    def _():
        for i in range(2):
            gw_ref[i, 0, :cols] = (acc_sc[i * cols:(i + 1) * cols] + gwi[i * cols:(i + 1) * cols]).astype(BF16)
            lo = 2 * cols + i * rows
            gw_ref[i, 0, cols:] = (acc_sc[lo:lo + rows] + gwo[i * rows:(i + 1) * rows]).astype(BF16)

    @pl.when(g == 0)
    def _():
        dh_sc[b] = d_h

    @pl.when(jnp.logical_and(g > 0, g < last))
    def _():
        dh_sc[b] += d_h

    @pl.when(g == last)
    def _():
        dh_ref[0] = dh_sc[b] + d_h


def block_forward(x_t, mod_cols, w_all, b_cols, qs, ks, cos_t, sin_t):
    n_b, dim, s_len = x_t.shape
    depth, n_t, n_j, piece, _ = w_all.shape
    cols = b_cols.shape[2]
    e = qs.shape[0]
    n_g = (n_t // 2) * n_j
    half = n_t // 2
    last = n_g - 1

    def ends(g, b):
        return jnp.where(jnp.logical_or(g == 0, g == last), b, n_b - 1)

    full = lambda *shape: pl.BlockSpec(shape, lambda g, b: (0,) * len(shape))
    head4 = lambda n, m: pl.BlockSpec((2, 1, n, m), lambda g, b: (g % half, g // half, 0, 0))
    head5 = lambda n, m: pl.BlockSpec((1, 2, 1, n, m), lambda g, b: (b, g % half, g // half, 0, 0))
    flops = 2 * n_b * s_len * dim * (n_t * n_j) * (cols + dim - cols) + 4 * n_b * n_t * n_j * s_len * s_len * e * 4
    return pl.pallas_call(
        functools.partial(fwd_kernel, e),
        grid=(n_g, n_b),
        in_specs=[
            pl.BlockSpec((1, dim, s_len), lambda g, b: (ends(g, b), 0, 0)),
            pl.BlockSpec((1, dim, 4), lambda g, b: (b, 0, 0)),
            pl.BlockSpec((depth, 2, 1, piece, dim), lambda g, b: (0, g % half, g // half, 0, 0)),
            head4(cols, 1),
            full(e, 1), full(e, 1), full(e // 2, s_len), full(e // 2, s_len),
        ],
        out_specs=[
            head5(cols, s_len),
            head5(e, s_len),
            pl.BlockSpec((1, 1, 2, s_len), lambda g, b: (b, g, 0, 0)),
            pl.BlockSpec((1, dim, s_len), lambda g, b: (jnp.where(g == 0, b, n_b - 1), 0, 0)),
            pl.BlockSpec((1, dim, s_len), lambda g, b: (jnp.where(g == last, b, 0), 0, 0)),
            pl.BlockSpec((1, dim, s_len), lambda g, b: (jnp.where(g == last, b, 0), 0, 0)),
        ],
        out_shape=[
            jax.ShapeDtypeStruct((n_b, n_t, n_j, cols, s_len), F32),
            jax.ShapeDtypeStruct((n_b, n_t, n_j, e, s_len), BF16),
            jax.ShapeDtypeStruct((n_b, n_g, 2, s_len), F32),
            jax.ShapeDtypeStruct((n_b, dim, s_len), BF16),
            jax.ShapeDtypeStruct((n_b, dim, s_len), F32),
            jax.ShapeDtypeStruct((n_b, dim, s_len), BF16),
        ],
        scratch_shapes=[pltpu.VMEM((n_b, dim, s_len), F32), pltpu.VMEM((n_b, dim, s_len), BF16)],
        compiler_params=pltpu.CompilerParams(dimension_semantics=("arbitrary", "arbitrary"), vmem_limit_bytes=63 * 1024 * 1024),
        cost_estimate=pl.CostEstimate(flops=flops, bytes_accessed=100_000_000, transcendentals=n_b * n_t * n_j * s_len * s_len),
        name="block_fwd",
    )(x_t, mod_cols, w_all, b_cols, qs, ks, cos_t, sin_t)


def block_backward(j_lo, j_n, d_br, h_t, w_all, qs, ks, cos_t, sin_t, y, o, lse):
    n_b, dim, s_len = d_br.shape
    depth, n_t, n_j, piece, _ = w_all.shape
    cols = y.shape[3]
    e = qs.shape[0]
    rows = dim - cols
    half = n_t // 2
    n_g = half * j_n

    full = lambda *shape: pl.BlockSpec(shape, lambda g, b: (0,) * len(shape))
    head5 = lambda n, m: pl.BlockSpec((1, 2, 1, n, m), lambda g, b: (b, g % half, j_lo + g // half, 0, 0))
    act = pl.BlockSpec((1, dim, s_len), lambda g, b: (b, 0, 0))
    flops = 4 * n_b * s_len * dim * (n_t * j_n) * dim + 10 * n_b * n_t * j_n * s_len * s_len * e * 4
    return pl.pallas_call(
        functools.partial(bwd_kernel, e),
        grid=(n_g, n_b),
        in_specs=[
            act, act,
            pl.BlockSpec((depth, 2, 1, piece, dim), lambda g, b: (0, g % half, j_lo + g // half, 0, 0)),
            full(e, 1), full(e, 1), full(e // 2, s_len), full(e // 2, s_len),
            head5(cols, s_len),
            head5(e, s_len),
            pl.BlockSpec((1, 1, 2, s_len), lambda g, b: (b, half * j_lo + g, 0, 0)),
        ],
        out_specs=[
            pl.BlockSpec((2, 1, dim, dim), lambda g, b: (g % half, g // half, 0, 0)),
            pl.BlockSpec((2, 1, cols, 1), lambda g, b: (g % half, g // half, 0, 0)),
            full(e, 1), full(e, 1),
            pl.BlockSpec((1, dim, s_len), lambda g, b: (jnp.where(g == n_g - 1, b, 0), 0, 0)),
        ],
        out_shape=[
            jax.ShapeDtypeStruct((n_t, j_n, dim, dim), BF16),
            jax.ShapeDtypeStruct((n_t, j_n, cols, 1), F32),
            jax.ShapeDtypeStruct((e, 1), F32),
            jax.ShapeDtypeStruct((e, 1), F32),
            jax.ShapeDtypeStruct((n_b, dim, s_len), F32),
        ],
        scratch_shapes=[
            pltpu.VMEM((n_b, dim, s_len), F32),
            pltpu.VMEM((2 * dim, dim), F32),
            pltpu.VMEM((2 * rows, s_len), BF16),
            pltpu.VMEM((2 * cols, s_len), BF16),
            pltpu.VMEM((2 * rows, s_len), BF16),
        ],
        compiler_params=pltpu.CompilerParams(dimension_semantics=("arbitrary", "arbitrary"), vmem_limit_bytes=63 * 1024 * 1024),
        cost_estimate=pl.CostEstimate(flops=flops, bytes_accessed=100_000_000, transcendentals=n_b * n_t * j_n * s_len * s_len),
        name="block_bwd",
    )(d_br, h_t, w_all, qs, ks, cos_t, sin_t, y, o, lse)


def swap_to_samples(arr, n):
    me = lax.axis_index("tp")
    k, s = arr.shape[0] // n, arr.shape[2]
    out = jnp.zeros((k, arr.shape[1], n * s), arr.dtype)
    own = lax.dynamic_slice_in_dim(arr, me * k, k, 0)
    out = lax.dynamic_update_slice_in_dim(out, own, me * s, 2)
    for step in range(1, n):
        peer = me ^ step
        got = lax.ppermute(lax.dynamic_slice_in_dim(arr, peer * k, k, 0), "tp", [(i, i ^ step) for i in range(n)])
        out = lax.dynamic_update_slice_in_dim(out, got, peer * s, 2)
    return out


def swap_to_tokens(arr, n):
    me = lax.axis_index("tp")
    k, s = arr.shape[0], arr.shape[2] // n
    out = jnp.zeros((n * k, arr.shape[1], s), arr.dtype)
    own = lax.dynamic_slice_in_dim(arr, me * s, s, 2)
    out = lax.dynamic_update_slice_in_dim(out, own, me * k, 0)
    for step in range(1, n):
        peer = me ^ step
        got = lax.ppermute(lax.dynamic_slice_in_dim(arr, peer * s, s, 2), "tp", [(i, i ^ step) for i in range(n)])
        out = lax.dynamic_update_slice_in_dim(out, got, peer * k, 0)
    return out


def pair_split(e):
    return np.concatenate([np.arange(0, e, 2), np.arange(1, e, 2)])


def solution(mesh):
    n_tp = mesh.shape["tp"]
    act_spec = P("dp", "tp", None)
    in_specs = (act_spec, P("dp", None), P("tp", None), P("tp", None), P(None, None, None), P(None, None), P(None, None, "tp", None), P(None, "tp", None), P(None, None), P(None, None), P(None, "tp", None, None), P(None, None), act_spec)
    out_specs = (act_spec, act_spec, P("dp", None, None), P("dp", None), P("dp", None, "tp", None), P("dp", "tp", None), P("dp", None), P("dp", None), P("dp", "tp", None, None), P("dp", None))

    def device_fn(x_in, cond_vec, rope_cos, rope_sin, w_mod, b_mod, w_in, b_in, q_scale, k_scale, w_out, b_out, d_out):
        n_l, dim, n_j, cols = w_in.shape
        e = q_scale.shape[1]
        rows = w_out.shape[2]
        n_all = x_in.shape[0]
        n_b = n_all // n_tp
        me = lax.axis_index("tp")
        order = pair_split(e)
        perm = np.concatenate([order, e + order, np.arange(2 * e, cols)])
        perm_mat = jnp.asarray(np.eye(cols, dtype=np.float32)[perm], BF16)

        w_in_t = jnp.einsum("ec,ldhc->lhed", perm_mat, w_in, preferred_element_type=F32).astype(BF16)
        w_local = jnp.concatenate([w_in_t, w_out], axis=2)
        w_full = [lax.all_gather(w_local[l], "tp", axis=0, tiled=False)[None] for l in range(n_l)]

        x_t = swap_to_samples(jnp.swapaxes(x_in, 1, 2), n_tp)
        g_t = swap_to_samples(jnp.swapaxes(d_out, 1, 2), n_tp)
        small_in = jnp.concatenate([rope_cos.T, rope_sin.T], axis=0)
        b_in_all = lax.all_gather(b_in, "tp", axis=0, tiled=False)
        tables = lax.all_gather(small_in, "tp", axis=1, tiled=True)
        cos_t, sin_t = tables[:e // 2], tables[e // 2:]
        b_cols = jnp.moveaxis(b_in_all, 1, 0).astype(F32)[..., perm, None]

        silu_all = jax.nn.silu(cond_vec.astype(F32)).astype(BF16)
        silu_own = lax.dynamic_slice_in_dim(silu_all, me * n_b, n_b, 0)
        mod = jnp.einsum("bd,ldm->lbm", silu_own, w_mod, preferred_element_type=F32) + b_mod.astype(F32)[:, None, :]
        shift, scale, gate = jnp.split(mod, 3, axis=-1)
        bias = jnp.broadcast_to(b_out.astype(F32)[:, None, :], shift.shape)
        mod_cols = jnp.stack([shift, scale, gate, bias], axis=-1)
        qs = q_scale.astype(F32)[:, order, None]
        ks = k_scale.astype(F32)[:, order, None]

        saved = []
        for l in range(n_l):
            y, o, lse, h_t, branch, x_new = block_forward(x_t, mod_cols[l], w_full[l], b_cols[l], qs[l], ks[l], cos_t, sin_t)
            saved.append((x_t, y, o, lse, h_t, branch))
            x_t = x_new
        x_out = jnp.swapaxes(swap_to_tokens(x_t, n_tp), 1, 2)

        grads = [None] * n_l
        small = [None] * n_l
        for l in reversed(range(n_l)):
            x_t, y, o, lse, h_t, branch = saved[l]
            g32 = g_t.astype(F32)
            d_gate = jnp.sum(g32 * branch, axis=2)
            gated = g32 * gate[l][:, :, None]
            d_bout = jnp.sum(gated, axis=(0, 2))
            d_br = gated.astype(BF16)
            d_h, d_qs, d_ks, gb, gw = 0.0, 0.0, 0.0, [], []
            for j in range(n_j):
                gw_j, gb_j, dq_j, dk_j, dh_j = block_backward(j, 1, d_br, h_t, w_full[l], qs[l], ks[l], cos_t, sin_t, y, o, lse)
                d_h, d_qs, d_ks = d_h + dh_j, d_qs + dq_j, d_ks + dk_j
                gb.append(gb_j)
                gw.append(lax.psum_scatter(gw_j[:, 0], "tp", scatter_dimension=0, tiled=False))
            x32 = x_t.astype(F32)
            cent = x32 - jnp.mean(x32, axis=1, keepdims=True)
            inv = lax.rsqrt(jnp.mean(cent * cent, axis=1, keepdims=True) + NORM_EPS)
            hat = cent * inv
            d_shift = jnp.sum(d_h, axis=2)
            d_scale = jnp.sum(d_h * hat, axis=2)
            d_hat = d_h * (1.0 + scale[l])[:, :, None]
            d_x = inv * (d_hat - jnp.mean(d_hat, axis=1, keepdims=True) - hat * jnp.mean(d_hat * hat, axis=1, keepdims=True))
            g_t = (g32 + d_x).astype(BF16)
            grads[l] = jnp.stack(gw)
            d_mod = jnp.concatenate([d_shift, d_scale, d_gate], axis=-1)
            small[l] = jnp.concatenate([d_mod.reshape(-1), d_bout, d_qs[:, 0], d_ks[:, 0], jnp.concatenate(gb, axis=1).reshape(-1)])

        grad_x = jnp.swapaxes(swap_to_tokens(g_t, n_tp), 1, 2)
        gathered = lax.all_gather(jnp.stack(small), "tp", axis=0, tiled=False)
        n_mod = n_b * 3 * dim
        d_mod = jnp.moveaxis(gathered[:, :, :n_mod].reshape(n_tp, n_l, n_b, 3 * dim), 1, 0).reshape(n_l, n_all, 3 * dim)
        sums = jnp.sum(gathered[:, :, n_mod:], axis=0)
        g_wmod = jnp.einsum("bd,lbm->ldm", silu_all.astype(F32), d_mod, preferred_element_type=F32)
        g_bmod = jnp.sum(d_mod, axis=1)
        inverse = np.argsort(order)
        g_bout = sums[:, :dim]
        g_qs = sums[:, dim:dim + e][:, inverse]
        g_ks = sums[:, dim + e:dim + 2 * e][:, inverse]
        g_bin = lax.dynamic_index_in_dim(sums[:, dim + 2 * e:].reshape(n_l, n_tp, n_j, cols), me, 1, keepdims=False)[..., np.argsort(perm)]
        gw_all = jnp.stack(grads)
        g_win = jnp.einsum("ec,lhed->ldhc", perm_mat, gw_all[:, :, :cols], preferred_element_type=F32).astype(BF16)
        g_wout = gw_all[:, :, cols:]
        return (x_out, grad_x, g_wmod, g_bmod, g_win, g_bin, g_qs, g_ks, g_wout, g_bout)

    return jax.shard_map(device_fn, mesh=mesh, in_specs=in_specs, out_specs=out_specs, check_vma=False)
```

```python
import functools
import jax
import jax.numpy as jnp
import numpy as np
from jax import lax
from jax.experimental import pallas as pl
from jax.experimental.pallas import tpu as pltpu
from jax.sharding import PartitionSpec as P

NORM_EPS = 1e-6
LOG2E = 1.4426950408889634
GELU_C = 0.7978845608028654
GELU_A = 0.044715
F32 = jnp.float32
BF16 = jnp.bfloat16
CHUNK = 256
VMEM = 63 * 1024 * 1024


def dot_nn(a, b):
    return lax.dot_general(a, b, (((1,), (0,)), ((), ())), preferred_element_type=F32)


def dot_nt(a, b):
    return lax.dot_general(a, b, (((1,), (1,)), ((), ())), preferred_element_type=F32)


def dot_tn(a, b):
    return lax.dot_general(a, b, (((0,), (0,)), ((), ())), preferred_element_type=F32)


def norm_rope(raw, scale_col, cos_t, sin_t):
    half = raw.shape[0] // 2
    inv = lax.rsqrt(jnp.mean(raw * raw, axis=0, keepdims=True) + NORM_EPS)
    hat = raw * inv
    scaled = hat * scale_col
    a, b = scaled[:half], scaled[half:]
    rot = jnp.concatenate([a * cos_t - b * sin_t, a * sin_t + b * cos_t], axis=0)
    return hat, inv, rot.astype(BF16)


def norm_rope_bwd(d_rot, hat, inv, scale_col, cos_t, sin_t):
    half = d_rot.shape[0] // 2
    da, db = d_rot[:half], d_rot[half:]
    d_scaled = jnp.concatenate([da * cos_t + db * sin_t, db * cos_t - da * sin_t], axis=0)
    d_scale = jnp.sum(d_scaled * hat, axis=1, keepdims=True)
    d_hat = d_scaled * scale_col
    d_raw = inv * (d_hat - hat * jnp.mean(d_hat * hat, axis=0, keepdims=True))
    return d_raw, d_scale


def softmax_head(q_rot, k_rot, v_t, o_ref, lse_ref, i, mul):
    n_c = q_rot.shape[1] // CHUNK
    spans = [slice(c * CHUNK, (c + 1) * CHUNK) for c in range(n_c)]
    nxt = dot_tn(k_rot, q_rot[:, spans[0]])
    outs = []
    for c in range(n_c):
        s = nxt
        if c + 1 < n_c:
            nxt = dot_tn(k_rot, q_rot[:, spans[c + 1]])
        top = jnp.max(s, axis=0, keepdims=True) * mul
        p = jnp.exp2(s * mul - top)
        tot = jnp.sum(p, axis=0, keepdims=True)
        out = (dot_nn(v_t, p.astype(BF16)) * (1.0 / tot)).astype(BF16)
        o_ref[0, 0, i, 0, :, spans[c]] = out
        outs.append(out)
        lse_ref[0, 0, 0, i:i + 1, spans[c]] = top + jnp.log2(tot)
    return jnp.concatenate(outs, axis=1)


def fwd_kernel(e, first, last, token_in, token_out, *refs):
    refs = list(refs)
    mod_ref, w_ref, bin_ref, qs_ref, ks_ref, cos_ref, sin_ref, x_ref = refs[:8]
    refs = refs[8:]
    if not first:
        h_in, z_in = refs[:2]
        refs = refs[5:]
    y_ref, o_ref, lse_ref = refs[:3]
    refs = refs[3:]
    if first:
        h_ref = refs.pop(0)
        if token_in:
            xt_ref = refs.pop(0)
    if last:
        br_ref, xo_ref = refs.pop(0), refs.pop(0)
    else:
        z_out = refs.pop(0)
    z_sc, h_sc = refs
    g, b = pl.program_id(0), pl.program_id(1)
    final = pl.num_programs(0) - 1
    cols = bin_ref.shape[2]

    @pl.when(g == 0)
    def _():
        if first:
            if token_in:
                x = jnp.concatenate([x_ref[t, 0].astype(F32).T for t in range(x_ref.shape[0])], axis=1)
                xt_ref[0] = x.astype(BF16)
            else:
                x = x_ref[0].astype(F32)
            cent = x - jnp.mean(x, axis=0, keepdims=True)
            normed = cent * lax.rsqrt(jnp.mean(cent * cent, axis=0, keepdims=True) + NORM_EPS)
            h = (normed * (1.0 + mod_ref[0, :, 1:2]) + mod_ref[0, :, 0:1]).astype(BF16)
            h_sc[b] = h
            h_ref[0] = h
        else:
            h_sc[b] = h_in[0]
            z_sc[b] = z_in[0]

    h_t = h_sc[b]
    cos_t, sin_t = cos_ref[...], sin_ref[...]
    mul = (e ** -0.5) * LOG2E
    joined = []
    ys = []
    for i in range(2):
        y = dot_nn(w_ref[i, 0, :cols], h_t) + bin_ref[i, 0]
        y_ref[0, 0, i, 0] = y
        ys.append(y)
    for i in range(2):
        y = ys[i]
        q_rot = norm_rope(y[:e], qs_ref[...], cos_t, sin_t)[2]
        k_rot = norm_rope(y[e:2 * e], ks_ref[...], cos_t, sin_t)[2]
        joined.append(softmax_head(q_rot, k_rot, y[2 * e:3 * e].astype(BF16), o_ref, lse_ref, i, mul))
        u = y[3 * e:]
        t = jnp.tanh(GELU_C * (u + GELU_A * u * u * u))
        joined.append((0.5 * u * (1.0 + t)).astype(BF16))
    z = dot_tn(jnp.concatenate([w_ref[0, 0, cols:], w_ref[1, 0, cols:]], axis=0), jnp.concatenate(joined, axis=0))

    if first:
        @pl.when(g == 0)
        def _():
            z_sc[b] = z

        @pl.when(jnp.logical_and(g > 0, g < final))
        def _():
            z_sc[b] += z
    else:
        @pl.when(g < final)
        def _():
            z_sc[b] += z

    @pl.when(g == final)
    def _():
        total = z_sc[b] + z
        if last:
            branch = total + mod_ref[0, :, 3:4]
            br_ref[0] = branch
            x_new = x_ref[0].astype(F32) + mod_ref[0, :, 2:3] * branch
            if token_out:
                n_t, s_t = xo_ref.shape[0], xo_ref.shape[2]
                for t in range(n_t):
                    xo_ref[t, 0] = x_new[:, t * s_t:(t + 1) * s_t].T.astype(BF16)
            else:
                xo_ref[0] = x_new.astype(BF16)
        else:
            z_out[0] = total


def bwd_kernel(e, chip_ref, dbr_ref, h_ref, wa_ref, wb_ref, qs_ref, ks_ref, cos_ref, sin_ref, y_ref, o_ref, lse_ref, gw_ref, gb_ref, dqs_ref, dks_ref, dh_ref, dh_sc, acc_sc, dj_sc, dp_sc, jn_sc):
    g, b = pl.program_id(0), pl.program_id(1)
    last = pl.num_programs(0) - 1
    cols = y_ref.shape[4]
    rows = dj_sc.shape[0] // 2
    s_len = dbr_ref.shape[2]
    d_br = dbr_ref[0]
    cos_t, sin_t = cos_ref[...], sin_ref[...]
    scale = e ** -0.5
    mul = scale * LOG2E
    own = lax.rem(g, 2) == 0
    ws = [jnp.where(own, wa_ref[i, 0], wb_ref[i, 0]) for i in range(2)]
    for i in range(2):
        dj_sc[i * rows:(i + 1) * rows] = dot_nn(ws[i][cols:], d_br).astype(BF16)

    @pl.when(jnp.logical_and(g == 0, b == 0))
    def _():
        dqs_ref[...] = jnp.zeros_like(dqs_ref)
        dks_ref[...] = jnp.zeros_like(dks_ref)

    @pl.when(b == 0)
    def _():
        gb_ref[...] = jnp.zeros_like(gb_ref)

    for i in range(2):
        base = i * cols
        q_hat, q_inv, q_rot = norm_rope(y_ref[0, 0, i, 0, :e], qs_ref[...], cos_t, sin_t)
        k_hat, k_inv, k_rot = norm_rope(y_ref[0, 0, i, 0, e:2 * e], ks_ref[...], cos_t, sin_t)
        v_t = y_ref[0, 0, i, 0, 2 * e:3 * e].astype(BF16)
        o_t = o_ref[0, 0, i, 0]
        d_o = dj_sc[i * rows:i * rows + e]
        d_sum = jnp.sum(d_o.astype(F32) * o_t.astype(F32), axis=0, keepdims=True)
        d_q, d_k, d_v = [], None, None
        for c in range(s_len // CHUNK):
            span = slice(c * CHUNK, (c + 1) * CHUNK)
            s = dot_tn(k_rot, q_rot[:, span])
            p = jnp.exp2(s * mul - lse_ref[0, 0, 0, i:i + 1, span])
            d_p = dot_tn(v_t, d_o[:, span])
            d_s = (p * (d_p - d_sum[:, span])).astype(BF16)
            d_q.append(dot_nn(k_rot, d_s))
            kc = dot_nt(q_rot[:, span], d_s)
            vc = dot_nt(d_o[:, span], p.astype(BF16))
            d_k = kc if d_k is None else d_k + kc
            d_v = vc if d_v is None else d_v + vc
        d_q = jnp.concatenate(d_q, axis=1) * scale
        d_qraw, d_qs = norm_rope_bwd(d_q, q_hat, q_inv, qs_ref[...], cos_t, sin_t)
        d_kraw, d_ks = norm_rope_bwd(d_k * scale, k_hat, k_inv, ks_ref[...], cos_t, sin_t)
        dqs_ref[...] += d_qs
        dks_ref[...] += d_ks
        u = y_ref[0, 0, i, 0, 3 * e:]
        t = jnp.tanh(GELU_C * (u + GELU_A * u * u * u))
        half = 0.5 * (1.0 + t)
        jn_sc[i * rows:i * rows + e] = o_t
        jn_sc[i * rows + e:(i + 1) * rows] = (u * half).astype(BF16)
        slope = half + 0.5 * u * (1.0 - t * t) * (GELU_C * (1.0 + 3.0 * GELU_A * u * u))
        d_u = dj_sc[i * rows + e:(i + 1) * rows].astype(F32) * slope
        off = 0
        for part in (d_qraw, d_kraw, d_v, d_u):
            n = part.shape[0]
            dp_sc[base + off:base + off + n] = part.astype(BF16)
            gb_ref[0, i, 0, off:off + n] += jnp.sum(part, axis=1, keepdims=True)
            off += n

    h_t = h_ref[0]
    gwi = dot_nt(dp_sc[...], h_t)
    gwo = dot_nt(jn_sc[...], d_br)
    d_h = dot_tn(jnp.concatenate([ws[0][:cols], ws[1][:cols]], axis=0), dp_sc[...])

    @pl.when(b == 0)
    def _():
        acc_sc[:2 * cols] = gwi
        acc_sc[2 * cols:] = gwo

    @pl.when(b > 0)
    def _():
        for i in range(2):
            gw_ref[0, i, 0, :cols] = (acc_sc[i * cols:(i + 1) * cols] + gwi[i * cols:(i + 1) * cols]).astype(BF16)
            lo = 2 * cols + i * rows
            gw_ref[0, i, 0, cols:] = (acc_sc[lo:lo + rows] + gwo[i * rows:(i + 1) * rows]).astype(BF16)

    @pl.when(g == 0)
    def _():
        dh_sc[b] = d_h

    @pl.when(jnp.logical_and(g > 0, g < last))
    def _():
        dh_sc[b] += d_h

    @pl.when(g == last)
    def _():
        dh_ref[0] = dh_sc[b] + d_h


def edge_kernel(has_exit, has_entry, token_g, token_out, *refs):
    refs = list(refs)
    g_ref = refs.pop(0)
    if has_exit:
        x_ref, mod_ref = refs.pop(0), refs.pop(0)
        dh_refs = [refs.pop(0) for _ in range(has_exit)]
    if has_entry:
        mod2_ref, br_ref = refs.pop(0), refs.pop(0)
    if has_exit:
        gx_ref, dmod_ref = refs.pop(0), refs.pop(0)
    if has_entry:
        if token_g:
            gt_ref = refs.pop(0)
        dbr_ref, dent_ref = refs.pop(0), refs.pop(0)
    if token_g:
        grad = jnp.concatenate([g_ref[t, 0].astype(F32).T for t in range(g_ref.shape[0])], axis=1)
        gt_ref[0] = grad.astype(BF16)
    else:
        grad = g_ref[0].astype(F32)
    if has_exit:
        d_h = dh_refs[0][0]
        for ref in dh_refs[1:]:
            d_h = d_h + ref[0]
        x = x_ref[0].astype(F32)
        cent = x - jnp.mean(x, axis=0, keepdims=True)
        inv = lax.rsqrt(jnp.mean(cent * cent, axis=0, keepdims=True) + NORM_EPS)
        hat = cent * inv
        dmod_ref[0, :, 0:1] = jnp.sum(d_h, axis=1, keepdims=True)
        dmod_ref[0, :, 1:2] = jnp.sum(d_h * hat, axis=1, keepdims=True)
        d_hat = d_h * (1.0 + mod_ref[0, :, 1:2])
        d_x = inv * (d_hat - jnp.mean(d_hat, axis=0, keepdims=True) - hat * jnp.mean(d_hat * hat, axis=0, keepdims=True))
        if token_out:
            s_t = gx_ref.shape[2]
            for t in range(gx_ref.shape[0]):
                span = slice(t * s_t, (t + 1) * s_t)
                gx_ref[t, 0] = (grad[:, span] + d_x[:, span]).T.astype(BF16)
        else:
            grad16 = (grad + d_x).astype(BF16)
            gx_ref[0] = grad16
            grad = grad16.astype(F32)
    if has_entry:
        dent_ref[0, :, 0:1] = jnp.sum(grad * br_ref[0], axis=1, keepdims=True)
        gated = grad * mod2_ref[0, :, 2:3]
        dent_ref[0, :, 1:2] = jnp.sum(gated, axis=1, keepdims=True)
        dbr_ref[0] = gated.astype(BF16)


def edge(grad, exit_args, entry_args, token_g, token_out):
    if token_g:
        n_t, n_b, s_t, dim = grad.shape
        s_len = n_t * s_t
    else:
        n_b, dim, s_len = grad.shape
    act = pl.BlockSpec((1, dim, s_len), lambda b: (b, 0, 0))
    small = lambda k: pl.BlockSpec((1, dim, k), lambda b: (b, 0, 0))
    tok = lambda n, s: pl.BlockSpec((n, 1, s, dim), lambda b: (0, b, 0, 0))
    args, in_specs, out_specs, out_shape = [grad], [tok(n_t, s_t) if token_g else act], [], []
    n_exit = 0
    if exit_args:
        x_t, mod_l, d_hs = exit_args
        n_exit = len(d_hs)
        args += [x_t, mod_l, *d_hs]
        in_specs += [act, small(4)] + [act] * n_exit
        if token_out:
            out_specs.append(tok(token_out, s_len // token_out))
            out_shape.append(jax.ShapeDtypeStruct((token_out, n_b, s_len // token_out, dim), BF16))
        else:
            out_specs.append(act)
            out_shape.append(jax.ShapeDtypeStruct((n_b, dim, s_len), BF16))
        out_specs.append(small(2))
        out_shape.append(jax.ShapeDtypeStruct((n_b, dim, 2), F32))
    if entry_args:
        mod_2, branch = entry_args
        args += [mod_2, branch]
        in_specs += [small(4), act]
        if token_g:
            out_specs.append(act)
            out_shape.append(jax.ShapeDtypeStruct((n_b, dim, s_len), BF16))
        out_specs += [act, small(2)]
        out_shape += [jax.ShapeDtypeStruct((n_b, dim, s_len), BF16), jax.ShapeDtypeStruct((n_b, dim, 2), F32)]
    return pl.pallas_call(
        functools.partial(edge_kernel, n_exit, bool(entry_args), token_g, token_out),
        grid=(n_b,), in_specs=in_specs, out_specs=out_specs, out_shape=out_shape,
        compiler_params=pltpu.CompilerParams(dimension_semantics=("arbitrary",), vmem_limit_bytes=VMEM),
        cost_estimate=pl.CostEstimate(flops=1_000_000, bytes_accessed=20_000_000, transcendentals=0),
        name="edge",
    )(*args)


def wmod_kernel(s_ref, d_ref, o_ref):
    o_ref[0] = dot_tn(s_ref[...], d_ref[0].astype(BF16))


def wmod_grad(silu_all, d_mod):
    n_l, n_all, width = d_mod.shape
    dim = silu_all.shape[1]
    piece = dim // 3
    return pl.pallas_call(
        wmod_kernel,
        grid=(n_l, 3),
        in_specs=[pl.BlockSpec((n_all, piece), lambda l, i: (0, i)), pl.BlockSpec((1, n_all, width), lambda l, i: (l, 0, 0))],
        out_specs=pl.BlockSpec((1, piece, width), lambda l, i: (l, i, 0)),
        out_shape=jax.ShapeDtypeStruct((n_l, dim, width), F32),
        compiler_params=pltpu.CompilerParams(dimension_semantics=("arbitrary", "arbitrary")),
        cost_estimate=pl.CostEstimate(flops=2 * n_l * n_all * dim * width, bytes_accessed=4 * n_l * dim * width, transcendentals=0),
        name="wmod_grad",
    )(silu_all, d_mod)


def block_forward(slot, x_in, mod_cols, w_pair, b_cols, qs, ks, cos_t, sin_t, prev, token_in, token_out):
    first, last = slot == 0, slot == 1
    token_in = token_in and first
    n_c, n_j, dim, _ = w_pair.shape
    cols = b_cols.shape[2]
    e = qs.shape[0]
    s_len = cos_t.shape[1]
    n_b = mod_cols.shape[0]
    final = n_j - 1
    full = lambda *shape: pl.BlockSpec(shape, lambda g, b: (0,) * len(shape))
    head6 = lambda n, m: pl.BlockSpec((1, 1, n_c, 1, n, m), lambda g, b: (b, slot, 0, g, 0, 0))
    act = lambda idx: pl.BlockSpec((1, dim, s_len), lambda g, b: (idx(g, b), 0, 0))
    at_start = lambda g, b: jnp.where(g == 0, b, n_b - 1)
    at_end = lambda g, b: jnp.where(g == final, b, 0)
    tok = lambda n, idx: pl.BlockSpec((n, 1, s_len // n, dim), lambda g, b: (0, idx(g, b), 0, 0))
    args = [mod_cols, w_pair, b_cols, qs, ks, cos_t, sin_t, x_in]
    in_specs = [
        pl.BlockSpec((1, dim, 4), lambda g, b: (b, 0, 0)),
        pl.BlockSpec((n_c, 1, dim, dim), lambda g, b: (0, g, 0, 0)),
        pl.BlockSpec((n_c, 1, cols, 1), lambda g, b: (0, g, 0, 0)),
        full(e, 1), full(e, 1), full(e // 2, s_len), full(e // 2, s_len),
        tok(x_in.shape[0], at_start) if token_in else act(at_start if first else at_end),
    ]
    aliases = {}
    if not first:
        y, o, lse, h_t, z = prev
        args += [h_t, z, y, o, lse]
        in_specs += [act(at_start), act(at_start)] + [pl.BlockSpec(memory_space=pl.ANY)] * 3
        aliases = {10: 0, 11: 1, 12: 2}
    out_specs = [head6(cols, s_len), head6(e, s_len), pl.BlockSpec((1, 1, 1, n_c, s_len), lambda g, b: (b, slot, g, 0, 0))]
    out_shape = [
        jax.ShapeDtypeStruct((n_b, 2, n_c, n_j, cols, s_len), F32),
        jax.ShapeDtypeStruct((n_b, 2, n_c, n_j, e, s_len), BF16),
        jax.ShapeDtypeStruct((n_b, 2, n_j, n_c, s_len), F32),
    ]
    shape16, shape32 = jax.ShapeDtypeStruct((n_b, dim, s_len), BF16), jax.ShapeDtypeStruct((n_b, dim, s_len), F32)
    if first:
        out_specs.append(act(at_start))
        out_shape.append(shape16)
        if token_in:
            out_specs.append(act(at_start))
            out_shape.append(shape16)
    if last:
        out_specs += [act(at_end), tok(token_out, at_end) if token_out else act(at_end)]
        out_shape += [shape32, jax.ShapeDtypeStruct((token_out, n_b, s_len // token_out, dim), BF16) if token_out else shape16]
    else:
        out_specs.append(act(at_end))
        out_shape.append(shape32)
    heads = n_c * n_j
    return pl.pallas_call(
        functools.partial(fwd_kernel, e, first, last, token_in, token_out),
        grid=(n_j, n_b), in_specs=in_specs, out_specs=out_specs, out_shape=out_shape,
        input_output_aliases=aliases,
        scratch_shapes=[pltpu.VMEM((n_b, dim, s_len), F32), pltpu.VMEM((n_b, dim, s_len), BF16)],
        compiler_params=pltpu.CompilerParams(dimension_semantics=("arbitrary", "arbitrary"), vmem_limit_bytes=VMEM),
        cost_estimate=pl.CostEstimate(flops=2 * n_b * heads * s_len * dim * dim + 16 * n_b * heads * s_len * s_len * e, bytes_accessed=60_000_000, transcendentals=n_b * heads * s_len * s_len),
        name="block_fwd",
    )(*args)


def block_backward(j_lo, j_n, chip, d_br, h_t, w_own, w_other, qs, ks, cos_t, sin_t, y, o, lse):
    n_b, dim, s_len = d_br.shape
    n_c = w_own.shape[0]
    cols = y.shape[4]
    e = qs.shape[0]
    rows = dim - cols
    n_g = 2 * j_n
    full = lambda *shape: pl.BlockSpec(shape, lambda g, b, c: (0,) * len(shape))
    head6 = lambda n, m: pl.BlockSpec((1, 1, n_c, 1, n, m), lambda g, b, c: (b, g % 2, 0, j_lo + g // 2, 0, 0))
    act = pl.BlockSpec((1, dim, s_len), lambda g, b, c: (b, 0, 0))
    pair = pl.BlockSpec((n_c, 1, dim, dim), lambda g, b, c: (0, j_lo + g // 2, 0, 0))
    grad = lambda n, m: pl.BlockSpec((1, n_c, 1, n, m), lambda g, b, c: (lax.rem(c[0] + g, 2), 0, g // 2, 0, 0))
    heads = 2 * n_c * j_n
    return pl.pallas_call(
        functools.partial(bwd_kernel, e),
        grid_spec=pltpu.PrefetchScalarGridSpec(
            num_scalar_prefetch=1,
            grid=(n_g, n_b),
            in_specs=[
                act, act, pair, pair,
                full(e, 1), full(e, 1), full(e // 2, s_len), full(e // 2, s_len),
                head6(cols, s_len), head6(e, s_len),
                pl.BlockSpec((1, 1, 1, n_c, s_len), lambda g, b, c: (b, g % 2, j_lo + g // 2, 0, 0)),
            ],
            out_specs=[
                grad(dim, dim), grad(cols, 1), full(e, 1), full(e, 1),
                pl.BlockSpec((1, dim, s_len), lambda g, b, c: (jnp.where(g == n_g - 1, b, 0), 0, 0)),
            ],
            scratch_shapes=[
                pltpu.VMEM((n_b, dim, s_len), F32),
                pltpu.VMEM((2 * dim, dim), F32),
                pltpu.VMEM((2 * rows, s_len), BF16),
                pltpu.VMEM((2 * cols, s_len), BF16),
                pltpu.VMEM((2 * rows, s_len), BF16),
            ],
        ),
        out_shape=[
            jax.ShapeDtypeStruct((2, n_c, j_n, dim, dim), BF16),
            jax.ShapeDtypeStruct((2, n_c, j_n, cols, 1), F32),
            jax.ShapeDtypeStruct((e, 1), F32),
            jax.ShapeDtypeStruct((e, 1), F32),
            jax.ShapeDtypeStruct((n_b, dim, s_len), F32),
        ],
        compiler_params=pltpu.CompilerParams(dimension_semantics=("arbitrary", "arbitrary"), vmem_limit_bytes=VMEM),
        cost_estimate=pl.CostEstimate(flops=4 * n_b * heads * s_len * dim * dim + 40 * n_b * heads * s_len * s_len * e, bytes_accessed=60_000_000, transcendentals=n_b * heads * s_len * s_len),
        name="block_bwd",
    )(chip, d_br, h_t, w_own, w_other, qs, ks, cos_t, sin_t, y, o, lse)


def even_first(arr, e):
    lead = arr.shape[:-1]
    return jnp.swapaxes(arr.reshape(*lead, e // 2, 2), -1, -2).reshape(*lead, e)


def interleave(arr, e):
    lead = arr.shape[:-1]
    return jnp.swapaxes(arr.reshape(*lead, 2, e // 2), -1, -2).reshape(*lead, e)


def pair_split(e):
    return np.concatenate([np.arange(0, e, 2), np.arange(1, e, 2)])


def solution(mesh):
    n_tp = mesh.shape["tp"]
    act_spec = P("dp", "tp", None)
    in_specs = (act_spec, P("dp", None), P("tp", None), P("tp", None), P(None, None, None), P(None, None), P(None, None, "tp", None), P(None, "tp", None), P(None, None), P(None, None), P(None, "tp", None, None), P(None, None), act_spec)
    out_specs = (act_spec, act_spec, P("dp", None, None), P("dp", None), P("dp", None, "tp", None), P("dp", "tp", None), P("dp", None), P("dp", None), P("dp", "tp", None, None), P("dp", None))
    same_chip = [[i, i + 1] for i in range(0, n_tp, 2)]
    across = [(i, (i + 2) % n_tp) for i in range(n_tp)]

    def device_step(x_in, cond_vec, rope_cos, rope_sin, w_mod, b_mod, w_in, b_in, q_scale, k_scale, w_out, b_out, d_out):
        n_l, dim, n_j, cols = w_in.shape
        e = q_scale.shape[1]
        n_all, s_own = x_in.shape[:2]
        n_b = n_all // n_tp
        me = lax.axis_index("tp")
        chip = me // 2
        order = pair_split(e)
        perm = np.concatenate([order, e + order, np.arange(2 * e, cols)])
        perm_mat = jnp.asarray(np.eye(cols, dtype=np.float32)[perm], BF16)

        n_rope = e * s_own
        b_perm = jnp.einsum("ec,lhc->lhe", perm_mat, b_in, preferred_element_type=F32)
        small_in = jnp.concatenate([rope_cos.T.reshape(-1), rope_sin.T.reshape(-1), b_perm.reshape(-1)])
        small_all = lax.all_gather(small_in, "tp", axis=0, tiled=False)
        small_all, x_in, w_in, w_out = lax.optimization_barrier((small_all, x_in, w_in, w_out))

        x_tok = lax.all_to_all(x_in.reshape(n_tp, n_b, s_own, dim), "tp", 0, 0)
        w_other, w_local = [], []
        for l in range(n_l):
            w_in_t = jnp.einsum("ec,dhc->hed", perm_mat, w_in[l], preferred_element_type=F32).astype(BF16)
            w_local.append(jnp.concatenate([w_in_t, w_out[l]], axis=1))
        gather_core = lambda w: lax.all_gather(w, "tp", axis=0, tiled=False, axis_index_groups=same_chip)
        w_own = [gather_core(w) for w in w_local]
        tie = x_tok

        tables = jnp.moveaxis(small_all[:, :n_rope].reshape(n_tp, e, s_own), 0, 1).reshape(e, n_tp * s_own)
        cos_t, sin_t = tables[:e // 2], tables[e // 2:]
        b_all = jnp.moveaxis(small_all[:, n_rope:].reshape(2, n_tp // 2, n_l, n_j, cols), 2, 0)[..., None]
        b_own = lax.dynamic_index_in_dim(b_all, chip, 1, keepdims=False)
        b_other = lax.dynamic_index_in_dim(b_all, 1 - chip, 1, keepdims=False)

        silu_all = jax.nn.silu(cond_vec.astype(F32)).astype(BF16)
        silu_own = lax.dynamic_slice_in_dim(silu_all, me * n_b, n_b, 0)
        mod = jnp.einsum("bd,ldm->lbm", silu_own, w_mod, preferred_element_type=F32) + b_mod.astype(F32)[:, None, :]
        bias = jnp.broadcast_to(b_out.astype(F32)[:, None, None, :], (n_l, n_b, 1, dim))
        mod_cols = jnp.swapaxes(jnp.concatenate([mod.reshape(n_l, n_b, 3, dim), bias], axis=2), 2, 3)
        qs = even_first(q_scale.astype(F32), e)[..., None]
        ks = even_first(k_scale.astype(F32), e)[..., None]

        saved = []
        x_cur = x_tok
        for l in range(n_l):
            consts = (qs[l], ks[l], cos_t, sin_t)
            mine, tie = lax.optimization_barrier((w_local[l], tie))
            if l == 0:
                x_cur = tie
            got = lax.ppermute(mine, "tp", across)
            half = block_forward(0, x_cur, mod_cols[l], w_own[l], b_own[l], *consts, None, l == 0, 0)
            y, o, lse, h_t = half[:4]
            x_t = half[4] if l == 0 else x_cur
            got, h_t = lax.optimization_barrier((got, h_t))
            tie = got
            w_other.append(gather_core(got))
            y, o, lse, branch, x_new = block_forward(1, x_t, mod_cols[l], w_other[l], b_other[l], *consts, (y, o, lse, h_t, half[-1]), False, n_tp if l == n_l - 1 else 0)
            saved.append((x_t, y, o, lse, h_t, branch))
            x_cur = x_new
        d_late, tie = lax.optimization_barrier((d_out, tie))
        g_tok = lax.all_to_all(d_late.reshape(n_tp, n_b, s_own, dim), "tp", 0, 0)
        x_out = lax.all_to_all(x_cur, "tp", 0, 0)

        grads = [None] * n_l
        d_mods = [None] * n_l
        small = [None] * n_l
        chip_arr = chip.astype(jnp.int32).reshape(1)
        top = n_l - 1
        g_t, d_br, d_ent = edge(g_tok, None, (mod_cols[top], saved[top][5]), True, 0)
        for l in reversed(range(n_l)):
            x_t, y, o, lse, h_t, branch = saved[l]
            splits = [(j, 1) for j in range(n_j)]
            if l == 0:
                d_br, x_out = lax.optimization_barrier((d_br, x_out))
            d_hs, d_qs, d_ks, gb, gw = [], 0.0, 0.0, [], []
            for j, width in splits:
                gw_j, gb_j, dq_j, dk_j, dh_j = block_backward(j, width, chip_arr, d_br, h_t, w_own[l], w_other[l], qs[l], ks[l], cos_t, sin_t, y, o, lse)
                d_hs.append(dh_j)
                d_qs, d_ks = d_qs + dq_j, d_ks + dk_j
                gb.append(gb_j)
                gw.append(lax.psum_scatter(gw_j.reshape(n_tp, width, dim, dim), "tp", scatter_dimension=0, tiled=False))
            entry = (mod_cols[l - 1], saved[l - 1][5]) if l > 0 else None
            edge_out = edge(g_t, (x_t, mod_cols[l], d_hs), entry, False, 0 if l > 0 else n_tp)
            d_out_cols = d_ent
            g_t, d_norm = edge_out[:2]
            if l > 0:
                d_br, d_ent = edge_out[2:]
            grads[l] = gw[0] if len(gw) == 1 else jnp.concatenate(gw, axis=0)
            d_mods[l] = jnp.swapaxes(jnp.concatenate([d_norm, d_out_cols[:, :, :1]], axis=2), 1, 2).reshape(n_b, 3 * dim)
            gb = gb[0] if len(gb) == 1 else jnp.concatenate(gb, axis=2)
            small[l] = jnp.concatenate([d_mods[l].reshape(-1), jnp.sum(d_out_cols[:, :, 1], axis=0), d_qs[:, 0], d_ks[:, 0], gb.reshape(-1)])

        grad_x = lax.all_to_all(g_t, "tp", 0, 0).reshape(n_all, s_own, dim)
        gathered = lax.all_gather(jnp.stack(small), "tp", axis=0, tiled=False)
        n_mod = n_b * 3 * dim
        d_mod = jnp.moveaxis(gathered[:, :, :n_mod].reshape(n_tp, n_l, n_b, 3 * dim), 1, 0).reshape(n_l, n_all, 3 * dim)
        sums = jnp.sum(gathered[:, :, n_mod:], axis=0)
        g_wmod = wmod_grad(silu_all, d_mod)
        g_bmod = jnp.sum(d_mod, axis=1)
        g_bout = sums[:, :dim]
        g_qs = interleave(sums[:, dim:dim + e], e)
        g_ks = interleave(sums[:, dim + e:dim + 2 * e], e)
        g_b = lax.dynamic_index_in_dim(sums[:, dim + 2 * e:].reshape(n_l, n_tp, n_j, cols), me, 1, keepdims=False)
        g_bin = jnp.concatenate([interleave(g_b[..., :e], e), interleave(g_b[..., e:2 * e], e), g_b[..., 2 * e:]], axis=-1)
        gw_all = jnp.stack(grads)
        g_win = jnp.einsum("ec,lhed->ldhc", perm_mat, gw_all[:, :, :cols], preferred_element_type=F32).astype(BF16)
        g_wout = gw_all[:, :, cols:]
        return (x_out.reshape(n_all, s_own, dim), grad_x, g_wmod, g_bmod, g_win, g_bin, g_qs, g_ks, g_wout, g_bout)

    return jax.shard_map(device_step, mesh=mesh, in_specs=in_specs, out_specs=out_specs, check_vma=False)
```

```python
import functools
import jax
import jax.numpy as jnp
import numpy as np
from jax import lax
from jax.experimental import pallas as pl
from jax.experimental.pallas import tpu as pltpu
from jax.sharding import PartitionSpec as P

NORM_EPS = 1e-6
LOG2E = 1.4426950408889634
GELU_C = 0.7978845608028654
GELU_A = 0.044715
F32 = jnp.float32
BF16 = jnp.bfloat16
CHUNK = 256
VMEM = 63 * 1024 * 1024
SPLIT = 4
SQ = pl.squeezed
FULL = ...
SMALL_FIRST = False


def dot_nn(a, b):
    return lax.dot_general(a, b, (((1,), (0,)), ((), ())), preferred_element_type=F32)


def dot_nt(a, b):
    return lax.dot_general(a, b, (((1,), (1,)), ((), ())), preferred_element_type=F32)


def dot_tn(a, b):
    return lax.dot_general(a, b, (((0,), (0,)), ((), ())), preferred_element_type=F32)


def norm_rope(raw, scale_col, cos_t, sin_t):
    half = raw.shape[0] // 2
    inv = lax.rsqrt(jnp.mean(raw * raw, axis=0, keepdims=True) + NORM_EPS)
    hat = raw * inv
    scaled = hat * scale_col
    a, b = scaled[:half], scaled[half:]
    rot = jnp.concatenate([a * cos_t - b * sin_t, a * sin_t + b * cos_t], axis=0)
    return hat, inv, rot.astype(BF16)


def norm_rope_bwd(d_rot, hat, inv, scale_col, cos_t, sin_t):
    half = d_rot.shape[0] // 2
    da, db = d_rot[:half], d_rot[half:]
    d_scaled = jnp.concatenate([da * cos_t + db * sin_t, db * cos_t - da * sin_t], axis=0)
    d_scale = jnp.sum(d_scaled * hat, axis=1, keepdims=True)
    d_hat = d_scaled * scale_col
    d_raw = inv * (d_hat - hat * jnp.mean(d_hat * hat, axis=0, keepdims=True))
    return d_raw, d_scale


def softmax_head(q_rot, k_rot, v_t, o_ref, lse_ref, i, mul, between):
    n_c = q_rot.shape[1] // CHUNK
    spans = [slice(c * CHUNK, (c + 1) * CHUNK) for c in range(n_c)]
    nxt = dot_tn(k_rot, q_rot[:, spans[0]])
    outs = []
    for c in range(n_c):
        s = nxt
        if c + 1 < n_c:
            nxt = dot_tn(k_rot, q_rot[:, spans[c + 1]])
        between(c, outs)
        top = jnp.max(s, axis=0, keepdims=True) * mul
        p = jnp.exp2(s * mul - top)
        tot = jnp.sum(p, axis=0, keepdims=True)
        out = (dot_nn(v_t, p.astype(BF16)) * (1.0 / tot)).astype(BF16)
        o_ref[i, :, spans[c]] = out
        outs.append(out)
        lse_ref[i:i + 1, spans[c]] = top + jnp.log2(tot)
    return jnp.concatenate(outs, axis=1)


def as_col(rows):
    return rows.T


def as_row(col):
    n = col.shape[0]
    return jnp.broadcast_to(col, (n, 128)).T[:1]


def from_tokens(ref):
    return jnp.concatenate([ref[t].astype(F32).T for t in range(ref.shape[0])], axis=1)


def gelu_parts(u):
    t = jnp.tanh(GELU_C * (u + GELU_A * u * u * u))
    return t, 0.5 * (1.0 + t)


def fwd_kernel(e, first, last, token_in, token_out, *refs):
    refs = list(refs)
    take = refs.pop
    mod_ref, wa_ref, wb_ref, bin_ref, qk_ref, cos_ref, sin_ref, x_ref = [take(0) for _ in range(8)]
    if not first:
        h_in, z_in = take(0), take(0)
        del refs[:3]
    y_ref, o_ref, lse_ref = take(0), take(0), take(0)
    if first:
        h_ref = take(0)
        if token_in:
            xt_ref = take(0)
    if last:
        br_ref = take(0)
        xo_ref = take(0)
    else:
        z_out = take(0)
    z_sc, h_sc, wo_sc = refs
    g, b = pl.program_id(0), pl.program_id(1)
    final = pl.num_programs(0) - 1
    cols = bin_ref.shape[-1]

    @pl.when(g == 0)
    def _():
        if first:
            mod = as_col(mod_ref[FULL])
            if token_in:
                x = from_tokens(x_ref)
                xt_ref[FULL] = x.astype(BF16)
            else:
                x = x_ref[FULL].astype(F32)
            cent = x - jnp.mean(x, axis=0, keepdims=True)
            normed = cent * lax.rsqrt(jnp.mean(cent * cent, axis=0, keepdims=True) + NORM_EPS)
            h = (normed * (1.0 + mod[:, 1:2]) + mod[:, :1]).astype(BF16)
            h_sc[b] = h
            h_ref[FULL] = h
            z_sc[b] = jnp.zeros_like(x)
        else:
            h_sc[b] = h_in[FULL]
            z_sc[b] = z_in[FULL]

    h_t = h_sc[b]
    cos_t, sin_t = cos_ref[FULL], sin_ref[FULL]
    q_col, k_col = [as_col(qk_ref[i])[:, :1] for i in range(2)]
    mul = (e ** -0.5) * LOG2E
    n_c = h_t.shape[1] // CHUNK
    spans = [slice(c * CHUNK, (c + 1) * CHUNK) for c in range(n_c)]
    bias = [as_col(bin_ref[i])[:, :1] for i in range(2)]
    wo_sc[FULL] = jnp.concatenate([wa_ref[cols:], wb_ref[cols:]], axis=0).T
    y_a = dot_nn(wa_ref[:cols], h_t) + bias[0]
    y_ref[0] = y_a

    def next_head(c, outs):
        y_ref[1, :, spans[c]] = dot_nn(wb_ref[:cols], h_t[:, spans[c]]) + bias[1]

    def attend(i, y, between):
        q_rot = norm_rope(y[:e], q_col, cos_t, sin_t)[-1]
        k_rot = norm_rope(y[e:2 * e], k_col, cos_t, sin_t)[-1]
        return softmax_head(q_rot, k_rot, y[2 * e:3 * e].astype(BF16), o_ref, lse_ref, i, mul, between)

    def mlp(u):
        return (u * gelu_parts(u)[1]).astype(BF16)

    def project(c, outs):
        tall = jnp.concatenate([o_a[:, spans[c]], m_a[:, spans[c]], outs[c], m_b[:, spans[c]]], axis=0)
        z_sc[b, :, spans[c]] += dot_nn(wo_sc[FULL], tall)

    def project_late(c, outs):
        if c > 0:
            project(c - 1, outs)

    o_a = attend(0, y_a, next_head)
    m_a = mlp(y_a[3 * e:])
    m_b = mlp(y_ref[1, 3 * e:])
    o_b = attend(1, y_ref[1, :3 * e], project_late)
    project(n_c - 1, [o_b[:, span] for span in spans])

    @pl.when(g == final)
    def _():
        if last:
            mod = as_col(mod_ref[FULL])
            branch = z_sc[b] + mod[:, 3:4]
            br_ref[FULL] = branch
            x_new = x_ref[FULL].astype(F32) + mod[:, 2:3] * branch
            if token_out:
                s_t = xo_ref.shape[1]
                for t in range(token_out):
                    xo_ref[t] = x_new[:, t * s_t:(t + 1) * s_t].T.astype(BF16)
            else:
                xo_ref[FULL] = x_new.astype(BF16)
        else:
            z_out[FULL] = z_sc[b]


def bwd_kernel(e, dbr_ref, h_ref, wa0_ref, wb0_ref, wa1_ref, wb1_ref, qk_ref, cos_ref, sin_ref, y_ref, o_ref, lse_ref, keep_ref, send_ref, gb_ref, dqk_ref, dh_ref, dh_sc, acc_sc, dj_sc, dp_new, jn_new, dp_sc, jn_sc, win_sc):
    step = pl.program_id(0)
    n = pl.num_programs(0) - 1
    cols = y_ref.shape[1]
    rows = dj_sc.shape[0] // 2
    s_len = dbr_ref.shape[-1]
    b = lax.rem(step, 2)
    scale = e ** -0.5
    mul = scale * LOG2E

    @pl.when(step == 0)
    def _():
        for ref in (dqk_ref, dh_sc, acc_sc, dp_sc, jn_sc, win_sc):
            ref[FULL] = jnp.zeros_like(ref)

    def dense():
        b_prev = 1 - b
        again = b_prev.astype(F32)
        gwi = dot_nt(dp_sc[FULL], h_ref[b_prev]) + again * acc_sc[:2 * cols]
        acc_sc[:2 * cols] = gwi
        gwo = dot_nt(jn_sc[FULL], dbr_ref[b_prev]) + again * acc_sc[2 * cols:]
        acc_sc[2 * cols:] = gwo
        for i, ref in enumerate((keep_ref, send_ref)):
            ref[:cols] = gwi[i * cols:(i + 1) * cols].astype(BF16)
            ref[cols:] = gwo[i * rows:(i + 1) * rows].astype(BF16)
        dh_sc[b_prev] += dot_nn(win_sc[FULL], dp_sc[FULL])

    def attention():
        own = lax.rem(step // 2, 2) == 0
        d_br = dbr_ref[b]
        cos_t, sin_t = cos_ref[FULL], sin_ref[FULL]
        q_col, k_col = [as_col(qk_ref[i])[:, :1] for i in range(2)]
        w_pair = [jnp.where(own, x[FULL], y[FULL]) for x, y in ((wa0_ref, wa1_ref), (wb0_ref, wb1_ref))]
        for i in range(2):
            dj_sc[i * rows:(i + 1) * rows] = dot_nn(w_pair[i][cols:], d_br).astype(BF16)
        sums = []
        for i in range(2):
            q_hat, q_inv, q_rot = norm_rope(y_ref[i, :e], q_col, cos_t, sin_t)
            k_hat, k_inv, k_rot = norm_rope(y_ref[i, e:2 * e], k_col, cos_t, sin_t)
            v_t = y_ref[i, 2 * e:3 * e].astype(BF16)
            o_t = o_ref[i]
            d_o = dj_sc[i * rows:i * rows + e]
            d_sum = jnp.sum(d_o.astype(F32) * o_t.astype(F32), axis=0, keepdims=True)
            d_q, d_k, d_v = [], 0.0, 0.0
            for c in range(s_len // CHUNK):
                span = slice(c * CHUNK, (c + 1) * CHUNK)
                p = jnp.exp2(dot_tn(k_rot, q_rot[:, span]) * mul - lse_ref[i:i + 1, span])
                d_p = dot_tn(v_t, d_o[:, span])
                d_s = (p * (d_p - d_sum[:, span])).astype(BF16)
                d_q.append(dot_nn(k_rot, d_s))
                d_k = d_k + dot_nt(q_rot[:, span], d_s)
                d_v = d_v + dot_nt(d_o[:, span], p.astype(BF16))
            d_qraw, d_qs = norm_rope_bwd(jnp.concatenate(d_q, axis=1) * scale, q_hat, q_inv, q_col, cos_t, sin_t)
            d_kraw, d_ks = norm_rope_bwd(d_k * scale, k_hat, k_inv, k_col, cos_t, sin_t)
            dqk_ref[0] += d_qs
            dqk_ref[1] += d_ks
            u = y_ref[i, 3 * e:]
            t, half = gelu_parts(u)
            jn_new[i * rows:i * rows + e] = o_t
            jn_new[i * rows + e:(i + 1) * rows] = (u * half).astype(BF16)
            slope = half + 0.5 * u * (1.0 - t * t) * (GELU_C * (1.0 + 3.0 * GELU_A * u * u))
            d_u = dj_sc[i * rows + e:(i + 1) * rows].astype(F32) * slope
            off = i * cols
            part_sums = []
            for part in (d_qraw, d_kraw, d_v, d_u):
                dp_new[off:off + part.shape[0]] = part.astype(BF16)
                part_sums.append(jnp.sum(part, axis=1, keepdims=True))
                off += part.shape[0]
            sums.append(as_row(jnp.concatenate(part_sums, axis=0)))
        for i in range(2):
            gb_ref[i] = jnp.where(b == 0, sums[i], gb_ref[i] + sums[i])
        return w_pair

    @pl.when(step < n)
    def _():
        dense()
        w_pair = attention()
        dp_sc[FULL] = dp_new[FULL]
        jn_sc[FULL] = jn_new[FULL]
        win_sc[FULL] = jnp.concatenate([w[:cols] for w in w_pair], axis=0).T

    @pl.when(step == n)
    def _():
        dense()

    @pl.when(step >= n - 1)
    def _():
        dh_ref[FULL] = dh_sc[1 - b]


def edge_kernel(n_exit, has_entry, token_g, token_out, *refs):
    refs = list(refs)
    take = refs.pop
    g_ref = take(0)
    if n_exit:
        x_ref, mod_ref = take(0), take(0)
        dh_refs = [take(0) for _ in range(n_exit)]
    if has_entry:
        mod2_ref, br_ref = take(0), take(0)
    if n_exit:
        gx_ref = take(0)
    if has_entry:
        if token_g:
            gt_ref = take(0)
        dbr_ref = take(0)
    sum_ref = take(0)
    grad = g_ref[FULL].astype(F32).T if token_g else g_ref[FULL].astype(F32)
    parts = []
    if n_exit:
        d_h = dh_refs[0][FULL]
        for ref in dh_refs[1:]:
            d_h = d_h + ref[FULL]
        x = x_ref[FULL].astype(F32)
        cent = x - jnp.mean(x, axis=0, keepdims=True)
        inv = lax.rsqrt(jnp.mean(cent * cent, axis=0, keepdims=True) + NORM_EPS)
        hat = cent * inv
        parts += [jnp.sum(d_h, axis=1, keepdims=True), jnp.sum(d_h * hat, axis=1, keepdims=True)]
        d_hat = d_h * (1.0 + as_col(mod_ref[FULL])[:, 1:2])
        d_x = inv * (d_hat - jnp.mean(d_hat, axis=0, keepdims=True) - hat * jnp.mean(d_hat * hat, axis=0, keepdims=True))
        grad = grad + d_x
        if token_out:
            gx_ref[FULL] = grad.T.astype(BF16)
        else:
            gx_ref[FULL] = grad.astype(BF16)
            grad = grad.astype(BF16).astype(F32)
    if has_entry:
        if token_g:
            gt_ref[FULL] = grad.astype(BF16)
        gated = grad * as_col(mod2_ref[FULL])[:, 2:3]
        parts += [jnp.sum(grad * br_ref[FULL], axis=1, keepdims=True), jnp.sum(gated, axis=1, keepdims=True)]
        dbr_ref[FULL] = gated.astype(BF16)

    @pl.when(pl.program_id(1) == 0)
    def _():
        sum_ref[FULL] = jnp.zeros_like(sum_ref)

    for i, part in enumerate(parts):
        sum_ref[i:i + 1] += as_row(part)


def params(n_axes):
    return pltpu.CompilerParams(dimension_semantics=("arbitrary",) * n_axes, vmem_limit_bytes=VMEM)


def shape_of(dtype, *shape):
    return jax.ShapeDtypeStruct(shape, dtype)


def edge(grad, exit_args, entry_args, token_g, token_out):
    if token_g:
        n_t, n_b, s_t, dim = grad.shape
    else:
        n_t, (n_b, dim, s_t) = SPLIT, grad.shape
        s_t = s_t // n_t
    act = pl.BlockSpec((SQ, dim, s_t), lambda b, t: (b, 0, t))
    rows = pl.BlockSpec((SQ, 8, dim), lambda b, t: (b, 0, 0))
    tok = pl.BlockSpec((SQ, SQ, s_t, dim), lambda b, t: (t, b, 0, 0))
    shape_act = shape_of(BF16, n_b, dim, n_t * s_t)
    args, in_specs, out_specs, out_shape = [grad], [tok if token_g else act], [], []
    if exit_args:
        x_t, mod_l, d_hs = exit_args
        args += [x_t, mod_l, *d_hs]
        in_specs += [act, rows] + [act] * len(d_hs)
        out_specs.append(tok if token_out else act)
        out_shape.append(shape_of(BF16, n_t, n_b, s_t, dim) if token_out else shape_act)
    if entry_args:
        args += entry_args
        in_specs += [rows, act]
        out_specs += [act] * (1 + token_g)
        out_shape += [shape_act] * (1 + token_g)
    return pl.pallas_call(
        functools.partial(edge_kernel, len(exit_args[2]) if exit_args else 0, bool(entry_args), token_g, token_out),
        grid=(n_b, n_t), in_specs=in_specs, out_specs=out_specs + [rows], out_shape=out_shape + [shape_of(F32, n_b, 8, dim)],
        compiler_params=params(2),
        cost_estimate=pl.CostEstimate(flops=10 ** 6, bytes_accessed=10 ** 7, transcendentals=0),
        name="edge",
    )(*args)


def wmod_kernel(s_ref, d_ref, o_ref):
    o_ref[FULL] = dot_tn(s_ref[FULL], d_ref[FULL].astype(BF16))


def wmod_grad(silu_all, d_mod):
    n_l, n_all, width = d_mod.shape
    dim = silu_all.shape[1]
    piece = dim // 3
    return pl.pallas_call(
        wmod_kernel,
        grid=(n_l, 3),
        in_specs=[pl.BlockSpec((n_all, piece), lambda l, i: (0, i)), pl.BlockSpec((SQ, n_all, width), lambda l, i: (l, 0, 0))],
        out_specs=pl.BlockSpec((SQ, piece, width), lambda l, i: (l, i, 0)),
        out_shape=shape_of(F32, n_l, dim, width),
        compiler_params=params(2),
        cost_estimate=pl.CostEstimate(flops=10 ** 6, bytes_accessed=10 ** 7, transcendentals=0),
        name="wmod_grad",
    )(silu_all, d_mod)


def block_forward(slot, x_in, mod_rows, w_pair, b_rows, qk, cos_t, sin_t, prev, token_in, token_out):
    first, last = slot == 0, slot == 1
    token_in = token_in and first
    n_j, dim = w_pair[0].shape[:2]
    n_c = len(w_pair)
    cols = b_rows.shape[-1]
    e = qk.shape[-1]
    s_len = cos_t.shape[1]
    n_b = mod_rows.shape[0]
    final = n_j - 1
    full = lambda *shape: pl.BlockSpec(shape, lambda g, b: (0,) * len(shape))
    head6 = lambda n, m: pl.BlockSpec((SQ, SQ, n_c, SQ, n, m), lambda g, b: (b, slot, 0, g, 0, 0))
    act = lambda idx: pl.BlockSpec((SQ, dim, s_len), lambda g, b: (idx(g, b), 0, 0))
    at_start = lambda g, b: jnp.where(g == 0, b, n_b - 1)
    at_end = lambda g, b: jnp.where(g == final, b, 0)
    tok = lambda n, idx: pl.BlockSpec((n, SQ, s_len // n, dim), lambda g, b: (0, idx(g, b), 0, 0))
    weight = pl.BlockSpec((SQ, dim, dim), lambda g, b: (g, 0, 0))
    args = [mod_rows, *w_pair, b_rows, qk, cos_t, sin_t, x_in]
    in_specs = [
        pl.BlockSpec((SQ, 8, dim), lambda g, b: (b, 0, 0)), weight, weight,
        pl.BlockSpec((n_c, SQ, 8, cols), lambda g, b: (0, g, 0, 0)),
        full(2, 8, e), full(e // 2, s_len), full(e // 2, s_len),
        tok(x_in.shape[0], at_start) if token_in else act(at_start if first else at_end),
    ]
    aliases = {}
    if not first:
        args += [prev[3], prev[4], *prev[:3]]
        in_specs += [act(at_start), act(at_start)] + [pl.BlockSpec(memory_space=pl.ANY)] * 3
        aliases = {len(args) - 3 + i: i for i in range(3)}
    shape16, shape32 = shape_of(BF16, n_b, dim, s_len), shape_of(F32, n_b, dim, s_len)
    out_specs = [head6(cols, s_len), head6(e, s_len), pl.BlockSpec((SQ, SQ, SQ, n_c, s_len), lambda g, b: (b, slot, g, 0, 0))]
    out_shape = [shape_of(F32, n_b, 2, n_c, n_j, cols, s_len), shape_of(BF16, n_b, 2, n_c, n_j, e, s_len), shape_of(F32, n_b, 2, n_j, n_c, s_len)]
    if first:
        out_specs += [act(at_start)] * (1 + token_in)
        out_shape += [shape16] * (1 + token_in)
    out_specs.append(act(at_end))
    out_shape.append(shape32)
    if last:
        out_specs.append(tok(token_out, at_end) if token_out else act(at_end))
        out_shape.append(shape_of(BF16, token_out, n_b, s_len // token_out, dim) if token_out else shape16)
    heads = n_c * n_j * n_b
    return pl.pallas_call(
        functools.partial(fwd_kernel, e, first, last, token_in, token_out),
        grid=(n_j, n_b), in_specs=in_specs, out_specs=out_specs, out_shape=out_shape,
        input_output_aliases=aliases,
        scratch_shapes=[pltpu.VMEM((n_b, dim, s_len), F32), pltpu.VMEM((n_b, dim, s_len), BF16), pltpu.VMEM((dim, 2 * (dim - cols)), BF16)],
        compiler_params=params(2),
        cost_estimate=pl.CostEstimate(flops=2 * heads * s_len * (dim * dim + 8 * s_len * e), bytes_accessed=10 ** 7, transcendentals=heads * s_len * s_len),
        name="block_fwd",
    )(*args)


def block_backward(j_lo, j_n, d_br, h_t, ws, qk, cos_t, sin_t, y, o, lse):
    n_b, dim, s_len = d_br.shape
    n_c, cols = y.shape[2], y.shape[4]
    e = qk.shape[-1]
    rows = dim - cols
    n = 2 * j_n * n_b
    group = lambda s: jnp.minimum(s, n - 1) // n_b
    before = lambda s: jnp.maximum(s - 1, 0) // n_b
    once = pl.Buffered(1)
    full = lambda *shape: pl.BlockSpec(shape, lambda s: (0,) * len(shape), pipeline_mode=once)
    head6 = lambda n_r, m: pl.BlockSpec((SQ, SQ, n_c, SQ, n_r, m), lambda s: (jnp.minimum(s, n - 1) % n_b, group(s) % 2, 0, j_lo + group(s) // 2, 0, 0))
    weight = pl.BlockSpec((SQ, dim, dim), lambda s: (j_lo + group(s) // 2, 0, 0))
    grad = pl.BlockSpec((SQ, SQ, dim, dim), lambda s: (before(s) % 2, before(s) // 2, 0, 0))
    heads = 2 * n_c * j_n * n_b
    return pl.pallas_call(
        functools.partial(bwd_kernel, e),
        grid=(n + 1,),
        in_specs=[
            full(n_b, dim, s_len), full(n_b, dim, s_len), weight, weight, weight, weight,
            full(2, 8, e), full(e // 2, s_len), full(e // 2, s_len),
            head6(cols, s_len), head6(e, s_len),
            pl.BlockSpec((SQ, SQ, SQ, n_c, s_len), lambda s: (jnp.minimum(s, n - 1) % n_b, group(s) % 2, j_lo + group(s) // 2, 0, 0)),
        ],
        out_specs=[
            grad, grad,
            pl.BlockSpec((n_c, SQ, SQ, 1, cols), lambda s: (0, group(s) % 2, group(s) // 2, 0, 0)),
            pl.BlockSpec((2, e, 1), lambda s: (0, 0, 0)),
            pl.BlockSpec((SQ, dim, s_len), lambda s: (jnp.where(s == n, 1, 0), 0, 0)),
        ],
        out_shape=[
            shape_of(BF16, 2, j_n, dim, dim), shape_of(BF16, 2, j_n, dim, dim),
            shape_of(F32, n_c, 2, j_n, 1, cols), shape_of(F32, 2, e, 1), shape_of(F32, n_b, dim, s_len),
        ],
        scratch_shapes=[
            pltpu.VMEM((n_b, dim, s_len), F32),
            pltpu.VMEM((2 * dim, dim), F32),
            pltpu.VMEM((2 * rows, s_len), BF16),
            pltpu.VMEM((2 * cols, s_len), BF16), pltpu.VMEM((2 * rows, s_len), BF16),
            pltpu.VMEM((2 * cols, s_len), BF16), pltpu.VMEM((2 * rows, s_len), BF16),
            pltpu.VMEM((dim, 2 * cols), BF16),
        ],
        compiler_params=params(1),
        cost_estimate=pl.CostEstimate(flops=4 * heads * s_len * (dim * dim + 10 * s_len * e), bytes_accessed=10 ** 7, transcendentals=heads * s_len * s_len),
        name="block_bwd",
    )(d_br, h_t, *ws, qk, cos_t, sin_t, y, o, lse)


def even_first(arr, e):
    lead = arr.shape[:-1]
    return jnp.swapaxes(arr.reshape(*lead, e // 2, 2), -1, -2).reshape(*lead, e)


def interleave(arr, e):
    lead = arr.shape[:-1]
    return jnp.swapaxes(arr.reshape(*lead, 2, e // 2), -1, -2).reshape(*lead, e)


def solution(mesh):
    n_tp = mesh.shape["tp"]
    act, part, heads1, heads2, whole = P("dp", "tp"), P("dp"), P(None, "tp"), P(None, None, "tp"), P()
    in_specs = (act, part, P("tp"), P("tp"), whole, whole, heads2, heads1, whole, whole, heads1, whole, act)
    out_specs = (act, act, part, part, P("dp", None, "tp"), act, part, part, act, part)
    peer_core = [(i, i ^ 1) for i in range(n_tp)]
    across = [(i, i ^ 2) for i in range(n_tp)]

    def swap(arr):
        return lax.all_to_all(arr, "tp", 0, 0)

    def device_step(x_in, cond_vec, rope_cos, rope_sin, w_mod, b_mod, w_in, b_in, q_scale, k_scale, w_out, b_out, d_out):
        n_l, dim, n_j, cols = w_in.shape
        e = q_scale.shape[1]
        n_all, s_own = x_in.shape[:2]
        n_b = n_all // n_tp
        me = lax.axis_index("tp")
        pairs = np.arange(e).reshape(e // 2, 2).T.reshape(-1)
        perm = np.concatenate([pairs, e + pairs, np.arange(2 * e, cols)])
        perm_mat = jnp.asarray(np.eye(cols, dtype=np.float32)[perm], BF16)

        n_rope = e * s_own
        b_perm = jnp.einsum("ec,lhc->lhe", perm_mat, b_in, preferred_element_type=F32)
        small_in = jnp.concatenate([rope_cos.T.reshape(-1), rope_sin.T.reshape(-1), b_perm.reshape(-1)])
        small_all = lax.all_gather(small_in, "tp", axis=0, tiled=False)
        small_all, x_in, w_in, w_out = lax.optimization_barrier((small_all, x_in, w_in, w_out))

        tie = swap(x_in.reshape(n_tp, n_b, s_own, dim))
        w_local = []
        for l in range(n_l):
            w_in_t = jnp.einsum("ec,dhc->hed", perm_mat, w_in[l], preferred_element_type=F32).astype(BF16)
            w_local.append(jnp.concatenate([w_in_t, w_out[l]], axis=1))
        w_own = [(w, lax.ppermute(w, "tp", peer_core)) for w in w_local]

        tables = jnp.moveaxis(small_all[:, :n_rope].reshape(n_tp, e, s_own), 0, 1).reshape(e, n_tp * s_own)
        cos_t, sin_t = tables[:e // 2], tables[e // 2:]
        b_all = small_all[:, n_rope:].reshape(n_tp, n_l, n_j, 1, cols)
        b_rel = jnp.stack([lax.dynamic_index_in_dim(b_all, me ^ i, 0, keepdims=False) for i in range(n_tp)])
        b_rel = jnp.broadcast_to(b_rel, (n_tp, n_l, n_j, 8, cols))

        silu_all = jax.nn.silu(cond_vec.astype(F32)).astype(BF16)
        silu_own = lax.dynamic_slice_in_dim(silu_all, me * n_b, n_b, 0)
        mod = jnp.einsum("bd,ldm->lbm", silu_own, w_mod, preferred_element_type=F32) + b_mod.astype(F32)[:, None]
        bias = jnp.broadcast_to(b_out.astype(F32)[:, None, None], (n_l, n_b, 5, dim))
        mod_rows = jnp.concatenate([mod.reshape(n_l, n_b, 3, dim), bias], axis=2)
        qk = even_first(jnp.stack([q_scale, k_scale], axis=1).astype(F32), e)
        qk = jnp.broadcast_to(qk[:, :, None], (n_l, 2, 8, e))

        saved, ws = [], []
        for l in range(n_l):
            consts = (qk[l], cos_t, sin_t)
            mine, tie = lax.optimization_barrier((w_local[l], tie))
            if l == 0:
                x_cur = tie
            got = lax.ppermute(mine, "tp", across)
            half = block_forward(0, x_cur, mod_rows[l], w_own[l], b_rel[:2, l], *consts, (), l == 0, 0)
            x_t = half[4] if l == 0 else x_cur
            got, h_t = lax.optimization_barrier((got, half[3]))
            tie = got
            w_other = (got, lax.ppermute(got, "tp", peer_core))
            y, o, lse, branch, x_cur = block_forward(1, x_t, mod_rows[l], w_other, b_rel[2:, l], *consts, (*half[:3], h_t, half[-1]), False, n_tp * (l == n_l - 1))
            saved.append((x_t, y, o, lse, h_t, branch))
            ws.append((*w_own[l], *w_other))
        d_late, tie = lax.optimization_barrier((d_out, tie))
        g_tok = swap(d_late.reshape(n_tp, n_b, s_own, dim))
        x_out = swap(x_cur)

        grads, small = [None] * n_l, [None] * n_l
        top = n_l - 1
        g_t, d_br, sums_in = edge(g_tok, (), (mod_rows[top], saved[top][5]), True, False)
        d_gate, d_bias = sums_in[:, 0], sums_in[:, 1]
        for l in reversed(range(n_l)):
            x_t, y, o, lse, h_t, branch = saved[l]
            if l == 0:
                d_br, x_out = lax.optimization_barrier((d_br, x_out))
            d_hs, d_qk, gb, gw = [], 0.0, [], []
            for j, width in ((0, n_j),) if l else ((0, n_j - 1), (n_j - 1, 1)):
                keep, send, gb_j, dqk_j, dh_j = block_backward(j, width, d_br, h_t, ws[l], qk[l], cos_t, sin_t, y, o, lse)
                d_hs.append(dh_j)
                d_qk = d_qk + dqk_j
                gb.append(gb_j)
                chip_sum = (keep.astype(F32) + lax.ppermute(send, "tp", peer_core).astype(F32)).astype(BF16)
                from_chip = lax.ppermute(chip_sum[1], "tp", across)
                gw.append((chip_sum[0].astype(F32) + from_chip.astype(F32)).astype(BF16))
            entry = (mod_rows[l - 1], saved[l - 1][5]) if l > 0 else ()
            edge_out = edge(g_t, (x_t, mod_rows[l], d_hs), entry, False, l == 0)
            g_t, sums = edge_out[0], edge_out[-1]
            grads[l] = jnp.concatenate(gw)
            d_mod = jnp.stack([sums[:, 0], sums[:, 1], d_gate], axis=1)
            gb = jnp.concatenate(gb, axis=2).reshape(2, 2, n_j * cols)
            gb = jnp.stack([lax.dynamic_index_in_dim(lax.dynamic_index_in_dim(gb, (i ^ me) % 2, 0, keepdims=False), (i ^ me) // 2, 0, keepdims=False) for i in range(n_tp)])
            small[l] = jnp.concatenate([d_mod.reshape(-1), jnp.sum(d_bias, axis=0), d_qk.reshape(-1), gb.reshape(-1)])
            if l > 0:
                d_br = edge_out[1]
                d_gate, d_bias = sums[:, 2], sums[:, 3]

        gathered = swap(jnp.broadcast_to(jnp.stack(small), (n_tp, n_l, small[0].shape[0])))
        g_t, gathered = lax.optimization_barrier((g_t, gathered)) if SMALL_FIRST else (g_t, gathered)
        grad_x = swap(g_t)
        n_mod = n_b * 3 * dim
        d_mod = jnp.moveaxis(gathered[:, :, :n_mod].reshape(n_tp, n_l, n_b, 3 * dim), 1, 0).reshape(n_l, n_all, 3 * dim)
        sums = jnp.sum(gathered[:, :, n_mod:], axis=0)
        g_wmod = wmod_grad(silu_all, d_mod)
        g_bmod = jnp.sum(d_mod, axis=1)
        g_qk = interleave(sums[:, dim:dim + 2 * e].reshape(n_l, 2, e), e)
        g_b = lax.dynamic_index_in_dim(sums[:, dim + 2 * e:].reshape(n_l, n_tp, n_j, cols), me, 1, keepdims=False)
        g_bin = jnp.concatenate([interleave(g_b[..., :e], e), interleave(g_b[..., e:2 * e], e), g_b[..., 2 * e:]], axis=-1)
        gw_all = jnp.stack(grads)
        g_win = jnp.einsum("ec,lhed->ldhc", perm_mat, gw_all[:, :, :cols], preferred_element_type=F32).astype(BF16)
        return (x_out.reshape(n_all, s_own, dim), grad_x.reshape(n_all, s_own, dim), g_wmod, g_bmod, g_win, g_bin, g_qk[:, 0], g_qk[:, 1], gw_all[:, :, cols:], sums[:, :dim])

    return jax.shard_map(device_step, mesh=mesh, in_specs=in_specs, out_specs=out_specs, check_vma=False)
```

```python
import functools
import jax
import jax.numpy as jnp
import numpy as np
from jax import lax
from jax.experimental import pallas as pl
from jax.experimental.pallas import tpu as pltpu
from jax.sharding import PartitionSpec as P

NORM_EPS = 1e-6
LOG2E = 1.4426950408889634
GELU_C = 0.7978845608028654
GELU_A = 0.044715
F32 = jnp.float32
BF16 = jnp.bfloat16
CHUNK = 512
VMEM = 63 * 1024 * 1024
SPLIT = 2
SQ = pl.squeezed
FULL = ...


def dot_nn(a, b):
    return lax.dot_general(a, b, (((1,), (0,)), ((), ())), preferred_element_type=F32)


def dot_nt(a, b):
    return lax.dot_general(a, b, (((1,), (1,)), ((), ())), preferred_element_type=F32)


def dot_tn(a, b):
    return lax.dot_general(a, b, (((0,), (0,)), ((), ())), preferred_element_type=F32)


def norm_rope(raw, scale_col, cos_t, sin_t):
    half = raw.shape[0] // 2
    inv = lax.rsqrt(jnp.mean(raw * raw, axis=0, keepdims=True) + NORM_EPS)
    hat = raw * inv
    scaled = hat * scale_col
    a, b = scaled[:half], scaled[half:]
    rot = jnp.concatenate([a * cos_t - b * sin_t, a * sin_t + b * cos_t], axis=0)
    return hat, inv, rot.astype(BF16)


def norm_rope_bwd(d_rot, hat, inv, scale_col, cos_t, sin_t):
    half = d_rot.shape[0] // 2
    da, db = d_rot[:half], d_rot[half:]
    d_scaled = jnp.concatenate([da * cos_t + db * sin_t, db * cos_t - da * sin_t], axis=0)
    d_scale = jnp.sum(d_scaled * hat, axis=1, keepdims=True)
    d_hat = d_scaled * scale_col
    d_raw = inv * (d_hat - hat * jnp.mean(d_hat * hat, axis=0, keepdims=True))
    return d_raw, d_scale


def softmax_head(q_rot, k_rot, v_t, o_ref, lse_ref, i, mul, between):
    n_c = q_rot.shape[1] // CHUNK
    spans = [slice(c * CHUNK, (c + 1) * CHUNK) for c in range(n_c)]
    nxt = dot_tn(k_rot, q_rot[:, spans[0]])
    outs = []
    for c in range(n_c):
        s = nxt
        if c + 1 < n_c:
            nxt = dot_tn(k_rot, q_rot[:, spans[c + 1]])
        between(c, outs)
        top = jnp.max(s, axis=0, keepdims=True) * mul
        p = jnp.exp2(s * mul - top)
        tot = jnp.sum(p, axis=0, keepdims=True)
        out = (dot_nn(v_t, p.astype(BF16)) * (1.0 / tot)).astype(BF16)
        o_ref[i, :, spans[c]] = out
        outs.append(out)
        lse_ref[i:i + 1, spans[c]] = top + jnp.log2(tot)
    return jnp.concatenate(outs, axis=1)


def as_col(rows):
    return rows.T


def as_row(col):
    n = col.shape[0]
    return jnp.broadcast_to(col, (n, 128)).T[:1]


def from_tokens(ref):
    return jnp.concatenate([ref[t].astype(F32).T for t in range(ref.shape[0])], axis=1)


def gelu_parts(u):
    t = jnp.tanh(GELU_C * (u + GELU_A * u * u * u))
    return t, 0.5 * (1.0 + t)


def fwd_kernel(e, first, last, token_in, token_out, *refs):
    refs = list(refs)
    take = refs.pop
    mod_ref, wa_ref, wb_ref, bin_ref, qk_ref, cos_ref, sin_ref, x_ref = [take(0) for _ in range(8)]
    if not first:
        h_in, z_in = take(0), take(0)
        del refs[:3]
    y_ref, o_ref, lse_ref = take(0), take(0), take(0)
    if first:
        h_ref = take(0)
        if token_in:
            xt_ref = take(0)
    if last:
        br_ref = take(0)
        xo_ref = take(0)
    else:
        z_out = take(0)
    z_sc, h_sc, wo_sc = refs
    g, b = pl.program_id(0), pl.program_id(1)
    final = pl.num_programs(0) - 1
    cols = bin_ref.shape[-1]

    @pl.when(g == 0)
    def _():
        if first:
            mod = as_col(mod_ref[FULL])
            if token_in:
                x = from_tokens(x_ref)
                xt_ref[FULL] = x.astype(BF16)
            else:
                x = x_ref[FULL].astype(F32)
            cent = x - jnp.mean(x, axis=0, keepdims=True)
            normed = cent * lax.rsqrt(jnp.mean(cent * cent, axis=0, keepdims=True) + NORM_EPS)
            h = (normed * (1.0 + mod[:, 1:2]) + mod[:, :1]).astype(BF16)
            h_sc[b] = h
            h_ref[FULL] = h
            z_sc[b] = jnp.zeros_like(x)
        else:
            h_sc[b] = h_in[FULL]
            z_sc[b] = z_in[FULL]

    h_t = h_sc[b]
    cos_t, sin_t = cos_ref[FULL], sin_ref[FULL]
    q_col, k_col = [as_col(qk_ref[i])[:, :1] for i in range(2)]
    mul = (e ** -0.5) * LOG2E
    n_c = h_t.shape[1] // CHUNK
    spans = [slice(c * CHUNK, (c + 1) * CHUNK) for c in range(n_c)]
    bias = [as_col(bin_ref[i])[:, :1] for i in range(2)]
    wo_sc[FULL] = jnp.concatenate([wa_ref[cols:], wb_ref[cols:]], axis=0).T
    y_a = dot_nn(wa_ref[:cols], h_t) + bias[0]
    y_ref[0] = y_a

    def next_head(c, outs):
        y_ref[1, :, spans[c]] = dot_nn(wb_ref[:cols], h_t[:, spans[c]]) + bias[1]

    def attend(i, y, between):
        q_rot = norm_rope(y[:e], q_col, cos_t, sin_t)[-1]
        k_rot = norm_rope(y[e:2 * e], k_col, cos_t, sin_t)[-1]
        return softmax_head(q_rot, k_rot, y[2 * e:3 * e].astype(BF16), o_ref, lse_ref, i, mul, between)

    def mlp(u):
        return (u * gelu_parts(u)[1]).astype(BF16)

    def project(c, outs):
        tall = jnp.concatenate([o_a[:, spans[c]], m_a[:, spans[c]], outs[c], m_b[:, spans[c]]], axis=0)
        z_sc[b, :, spans[c]] += dot_nn(wo_sc[FULL], tall)

    def project_late(c, outs):
        if c > 0:
            project(c - 1, outs)

    o_a = attend(0, y_a, next_head)
    m_a = mlp(y_a[3 * e:])
    m_b = mlp(y_ref[1, 3 * e:])
    o_b = attend(1, y_ref[1, :3 * e], project_late)
    project(n_c - 1, [o_b[:, span] for span in spans])

    @pl.when(g == final)
    def _():
        if last:
            mod = as_col(mod_ref[FULL])
            branch = z_sc[b] + mod[:, 3:4]
            br_ref[FULL] = branch
            x_new = x_ref[FULL].astype(F32) + mod[:, 2:3] * branch
            if token_out:
                s_t = xo_ref.shape[1]
                for t in range(token_out):
                    xo_ref[t] = x_new[:, t * s_t:(t + 1) * s_t].T.astype(BF16)
            else:
                xo_ref[FULL] = x_new.astype(BF16)
        else:
            z_out[FULL] = z_sc[b]


def bwd_kernel(e, dbr_ref, h_ref, wa0_ref, wb0_ref, wa1_ref, wb1_ref, qk_ref, cos_ref, sin_ref, y_ref, o_ref, lse_ref, keep_ref, send_ref, gb_ref, dqk_ref, dh_ref, dh_sc, acc_sc, dj_sc, dp_new, jn_new, dp_sc, jn_sc, win_sc):
    step = pl.program_id(0)
    n = pl.num_programs(0) - 1
    cols = y_ref.shape[1]
    rows = dj_sc.shape[0] // 2
    s_len = dbr_ref.shape[-1]
    b = lax.rem(step, 2)
    scale = e ** -0.5
    mul = scale * LOG2E

    @pl.when(step == 0)
    def _():
        for ref in (dqk_ref, dh_sc, acc_sc, dp_sc, jn_sc, win_sc):
            ref[FULL] = jnp.zeros_like(ref)

    def dense():
        b_prev = 1 - b
        again = b_prev.astype(F32)
        gwi = dot_nt(dp_sc[FULL], h_ref[b_prev]) + again * acc_sc[:2 * cols]
        acc_sc[:2 * cols] = gwi
        gwo = dot_nt(jn_sc[FULL], dbr_ref[b_prev]) + again * acc_sc[2 * cols:]
        acc_sc[2 * cols:] = gwo
        for i, ref in enumerate((keep_ref, send_ref)):
            ref[:cols] = gwi[i * cols:(i + 1) * cols].astype(BF16)
            ref[cols:] = gwo[i * rows:(i + 1) * rows].astype(BF16)
        dh_sc[b_prev] += dot_nn(win_sc[FULL], dp_sc[FULL])

    def attention():
        own = lax.rem(step // 2, 2) == 0
        d_br = dbr_ref[b]
        cos_t, sin_t = cos_ref[FULL], sin_ref[FULL]
        q_col, k_col = [as_col(qk_ref[i])[:, :1] for i in range(2)]
        w_pair = [jnp.where(own, x[FULL], y[FULL]) for x, y in ((wa0_ref, wa1_ref), (wb0_ref, wb1_ref))]
        for i in range(2):
            dj_sc[i * rows:(i + 1) * rows] = dot_nn(w_pair[i][cols:], d_br).astype(BF16)
        sums = []
        for i in range(2):
            q_hat, q_inv, q_rot = norm_rope(y_ref[i, :e], q_col, cos_t, sin_t)
            k_hat, k_inv, k_rot = norm_rope(y_ref[i, e:2 * e], k_col, cos_t, sin_t)
            v_t = y_ref[i, 2 * e:3 * e].astype(BF16)
            o_t = o_ref[i]
            d_o = dj_sc[i * rows:i * rows + e]
            d_sum = jnp.sum(d_o.astype(F32) * o_t.astype(F32), axis=0, keepdims=True)
            d_q, d_k, d_v = [], 0.0, 0.0
            for c in range(s_len // CHUNK):
                span = slice(c * CHUNK, (c + 1) * CHUNK)
                p = jnp.exp2(dot_tn(k_rot, q_rot[:, span]) * mul - lse_ref[i:i + 1, span])
                d_p = dot_tn(v_t, d_o[:, span])
                d_s = (p * (d_p - d_sum[:, span])).astype(BF16)
                d_q.append(dot_nn(k_rot, d_s))
                d_k = d_k + dot_nt(q_rot[:, span], d_s)
                d_v = d_v + dot_nt(d_o[:, span], p.astype(BF16))
            d_qraw, d_qs = norm_rope_bwd(jnp.concatenate(d_q, axis=1) * scale, q_hat, q_inv, q_col, cos_t, sin_t)
            d_kraw, d_ks = norm_rope_bwd(d_k * scale, k_hat, k_inv, k_col, cos_t, sin_t)
            dqk_ref[0] += d_qs
            dqk_ref[1] += d_ks
            u = y_ref[i, 3 * e:]
            t, half = gelu_parts(u)
            jn_new[i * rows:i * rows + e] = o_t
            jn_new[i * rows + e:(i + 1) * rows] = (u * half).astype(BF16)
            slope = half + 0.5 * u * (1.0 - t * t) * (GELU_C * (1.0 + 3.0 * GELU_A * u * u))
            d_u = dj_sc[i * rows + e:(i + 1) * rows].astype(F32) * slope
            off = i * cols
            part_sums = []
            for part in (d_qraw, d_kraw, d_v, d_u):
                dp_new[off:off + part.shape[0]] = part.astype(BF16)
                part_sums.append(jnp.sum(part, axis=1, keepdims=True))
                off += part.shape[0]
            sums.append(as_row(jnp.concatenate(part_sums, axis=0)))
        for i in range(2):
            gb_ref[i] = jnp.where(b == 0, sums[i], gb_ref[i] + sums[i])
        return w_pair

    @pl.when(step < n)
    def _():
        dense()
        w_pair = attention()
        dp_sc[FULL] = dp_new[FULL]
        jn_sc[FULL] = jn_new[FULL]
        win_sc[FULL] = jnp.concatenate([w[:cols] for w in w_pair], axis=0).T

    @pl.when(step == n)
    def _():
        dense()

    @pl.when(step >= n - 1)
    def _():
        dh_ref[FULL] = dh_sc[1 - b]


def edge_kernel(n_exit, has_entry, token_g, token_out, *refs):
    refs = list(refs)
    take = refs.pop
    g_ref = take(0)
    if n_exit:
        x_ref, mod_ref = take(0), take(0)
        dh_refs = [take(0) for _ in range(n_exit)]
    if has_entry:
        mod2_ref, br_ref = take(0), take(0)
    if n_exit:
        gx_ref = take(0)
    if has_entry:
        if token_g:
            gt_ref = take(0)
        dbr_ref = take(0)
    sum_ref = take(0)
    grad = from_tokens(g_ref) if token_g else g_ref[FULL].astype(F32)
    parts = []
    if n_exit:
        d_h = dh_refs[0][FULL]
        for ref in dh_refs[1:]:
            d_h = d_h + ref[FULL]
        x = x_ref[FULL].astype(F32)
        cent = x - jnp.mean(x, axis=0, keepdims=True)
        inv = lax.rsqrt(jnp.mean(cent * cent, axis=0, keepdims=True) + NORM_EPS)
        hat = cent * inv
        parts += [jnp.sum(d_h, axis=1, keepdims=True), jnp.sum(d_h * hat, axis=1, keepdims=True)]
        d_hat = d_h * (1.0 + as_col(mod_ref[FULL])[:, 1:2])
        d_x = inv * (d_hat - jnp.mean(d_hat, axis=0, keepdims=True) - hat * jnp.mean(d_hat * hat, axis=0, keepdims=True))
        grad = grad + d_x
        if token_out:
            s_t = gx_ref.shape[1]
            for t in range(gx_ref.shape[0]):
                gx_ref[t] = grad[:, t * s_t:(t + 1) * s_t].T.astype(BF16)
        else:
            gx_ref[FULL] = grad.astype(BF16)
            grad = grad.astype(BF16).astype(F32)
    if has_entry:
        if token_g:
            gt_ref[FULL] = grad.astype(BF16)
        gated = grad * as_col(mod2_ref[FULL])[:, 2:3]
        parts += [jnp.sum(grad * br_ref[FULL], axis=1, keepdims=True), jnp.sum(gated, axis=1, keepdims=True)]
        dbr_ref[FULL] = gated.astype(BF16)

    @pl.when(pl.program_id(1) == 0)
    def _():
        sum_ref[FULL] = jnp.zeros_like(sum_ref)

    for i, part in enumerate(parts):
        sum_ref[i:i + 1] += as_row(part)


def params(n_axes):
    return pltpu.CompilerParams(dimension_semantics=("arbitrary",) * n_axes, vmem_limit_bytes=VMEM)


def shape_of(dtype, *shape):
    return jax.ShapeDtypeStruct(shape, dtype)


def edge(grad, exit_args, entry_args, token_g, token_out):
    if token_g:
        n_t, n_b, s_t, dim = grad.shape
    else:
        n_t, (n_b, dim, s_t) = token_out or SPLIT, grad.shape
        s_t = s_t // n_t
    act = pl.BlockSpec((SQ, dim, n_t * s_t // SPLIT), lambda b, t: (b, 0, t))
    rows = pl.BlockSpec((SQ, 8, dim), lambda b, t: (b, 0, 0))
    tok = pl.BlockSpec((n_t // SPLIT, SQ, s_t, dim), lambda b, t: (t, b, 0, 0))
    shape_act = shape_of(BF16, n_b, dim, n_t * s_t)
    args, in_specs, out_specs, out_shape = [grad], [tok if token_g else act], [], []
    if exit_args:
        x_t, mod_l, d_hs = exit_args
        args += [x_t, mod_l, *d_hs]
        in_specs += [act, rows] + [act] * len(d_hs)
        out_specs.append(tok if token_out else act)
        out_shape.append(shape_of(BF16, n_t, n_b, s_t, dim) if token_out else shape_act)
    if entry_args:
        args += entry_args
        in_specs += [rows, act]
        out_specs += [act] * (1 + token_g)
        out_shape += [shape_act] * (1 + token_g)
    return pl.pallas_call(
        functools.partial(edge_kernel, len(exit_args[2]) if exit_args else 0, bool(entry_args), token_g, token_out),
        grid=(n_b, SPLIT), in_specs=in_specs, out_specs=out_specs + [rows], out_shape=out_shape + [shape_of(F32, n_b, 8, dim)],
        compiler_params=params(2),
        cost_estimate=pl.CostEstimate(flops=10 ** 6, bytes_accessed=10 ** 7, transcendentals=0),
        name="edge",
    )(*args)


def wmod_kernel(s_ref, d_ref, o_ref):
    o_ref[FULL] = dot_tn(s_ref[FULL], d_ref[FULL].astype(BF16))


def wmod_grad(silu_all, d_mod):
    n_l, n_all, width = d_mod.shape
    dim = silu_all.shape[1]
    piece = dim // 3
    return pl.pallas_call(
        wmod_kernel,
        grid=(n_l, 3),
        in_specs=[pl.BlockSpec((n_all, piece), lambda l, i: (0, i)), pl.BlockSpec((SQ, n_all, width), lambda l, i: (l, 0, 0))],
        out_specs=pl.BlockSpec((SQ, piece, width), lambda l, i: (l, i, 0)),
        out_shape=shape_of(F32, n_l, dim, width),
        compiler_params=params(2),
        cost_estimate=pl.CostEstimate(flops=10 ** 6, bytes_accessed=10 ** 7, transcendentals=0),
        name="wmod_grad",
    )(silu_all, d_mod)


def block_forward(slot, x_in, mod_rows, w_pair, b_rows, qk, cos_t, sin_t, prev, token_in, token_out):
    first, last = slot == 0, slot == 1
    token_in = token_in and first
    n_j, dim = w_pair[0].shape[:2]
    n_c = len(w_pair)
    cols = b_rows.shape[-1]
    e = qk.shape[-1]
    s_len = cos_t.shape[1]
    n_b = mod_rows.shape[0]
    final = n_j - 1
    full = lambda *shape: pl.BlockSpec(shape, lambda g, b: (0,) * len(shape))
    head6 = lambda n, m: pl.BlockSpec((SQ, SQ, n_c, SQ, n, m), lambda g, b: (b, slot, 0, g, 0, 0))
    act = lambda idx: pl.BlockSpec((SQ, dim, s_len), lambda g, b: (idx(g, b), 0, 0))
    at_start = lambda g, b: jnp.where(g == 0, b, n_b - 1)
    at_end = lambda g, b: jnp.where(g == final, b, 0)
    tok = lambda n, idx: pl.BlockSpec((n, SQ, s_len // n, dim), lambda g, b: (0, idx(g, b), 0, 0))
    weight = pl.BlockSpec((SQ, dim, dim), lambda g, b: (g, 0, 0))
    args = [mod_rows, *w_pair, b_rows, qk, cos_t, sin_t, x_in]
    in_specs = [
        pl.BlockSpec((SQ, 8, dim), lambda g, b: (b, 0, 0)), weight, weight,
        pl.BlockSpec((n_c, SQ, 8, cols), lambda g, b: (0, g, 0, 0)),
        full(2, 8, e), full(e // 2, s_len), full(e // 2, s_len),
        tok(x_in.shape[0], at_start) if token_in else act(at_start if first else at_end),
    ]
    aliases = {}
    if not first:
        args += [prev[3], prev[4], *prev[:3]]
        in_specs += [act(at_start), act(at_start)] + [pl.BlockSpec(memory_space=pl.ANY)] * 3
        aliases = {len(args) - 3 + i: i for i in range(3)}
    shape16, shape32 = shape_of(BF16, n_b, dim, s_len), shape_of(F32, n_b, dim, s_len)
    out_specs = [head6(cols, s_len), head6(e, s_len), pl.BlockSpec((SQ, SQ, SQ, n_c, s_len), lambda g, b: (b, slot, g, 0, 0))]
    out_shape = [shape_of(F32, n_b, 2, n_c, n_j, cols, s_len), shape_of(BF16, n_b, 2, n_c, n_j, e, s_len), shape_of(F32, n_b, 2, n_j, n_c, s_len)]
    if first:
        out_specs += [act(at_start)] * (1 + token_in)
        out_shape += [shape16] * (1 + token_in)
    out_specs.append(act(at_end))
    out_shape.append(shape32)
    if last:
        out_specs.append(tok(token_out, at_end) if token_out else act(at_end))
        out_shape.append(shape_of(BF16, token_out, n_b, s_len // token_out, dim) if token_out else shape16)
    heads = n_c * n_j * n_b
    return pl.pallas_call(
        functools.partial(fwd_kernel, e, first, last, token_in, token_out),
        grid=(n_j, n_b), in_specs=in_specs, out_specs=out_specs, out_shape=out_shape,
        input_output_aliases=aliases,
        scratch_shapes=[pltpu.VMEM((n_b, dim, s_len), F32), pltpu.VMEM((n_b, dim, s_len), BF16), pltpu.VMEM((dim, 2 * (dim - cols)), BF16)],
        compiler_params=params(2),
        cost_estimate=pl.CostEstimate(flops=2 * heads * s_len * (dim * dim + 8 * s_len * e), bytes_accessed=10 ** 7, transcendentals=heads * s_len * s_len),
        name="block_fwd",
    )(*args)


def block_backward(j_lo, j_n, d_br, h_t, ws, qk, cos_t, sin_t, y, o, lse):
    n_b, dim, s_len = d_br.shape
    n_c, cols = y.shape[2], y.shape[4]
    e = qk.shape[-1]
    rows = dim - cols
    n = 2 * j_n * n_b
    group = lambda s: jnp.minimum(s, n - 1) // n_b
    before = lambda s: jnp.maximum(s - 1, 0) // n_b
    once = pl.Buffered(1)
    full = lambda *shape: pl.BlockSpec(shape, lambda s: (0,) * len(shape), pipeline_mode=once)
    head6 = lambda n_r, m: pl.BlockSpec((SQ, SQ, n_c, SQ, n_r, m), lambda s: (jnp.minimum(s, n - 1) % n_b, group(s) % 2, 0, j_lo + group(s) // 2, 0, 0))
    weight = pl.BlockSpec((SQ, dim, dim), lambda s: (j_lo + group(s) // 2, 0, 0))
    grad = pl.BlockSpec((SQ, SQ, dim, dim), lambda s: (before(s) % 2, before(s) // 2, 0, 0))
    heads = 2 * n_c * j_n * n_b
    return pl.pallas_call(
        functools.partial(bwd_kernel, e),
        grid=(n + 1,),
        in_specs=[
            full(n_b, dim, s_len), full(n_b, dim, s_len), weight, weight, weight, weight,
            full(2, 8, e), full(e // 2, s_len), full(e // 2, s_len),
            head6(cols, s_len), head6(e, s_len),
            pl.BlockSpec((SQ, SQ, SQ, n_c, s_len), lambda s: (jnp.minimum(s, n - 1) % n_b, group(s) % 2, j_lo + group(s) // 2, 0, 0)),
        ],
        out_specs=[
            grad, grad,
            pl.BlockSpec((n_c, SQ, SQ, 1, cols), lambda s: (0, group(s) % 2, group(s) // 2, 0, 0)),
            pl.BlockSpec((2, e, 1), lambda s: (0, 0, 0)),
            pl.BlockSpec((SQ, dim, s_len), lambda s: (jnp.where(s == n, 1, 0), 0, 0)),
        ],
        out_shape=[
            shape_of(BF16, 2, j_n, dim, dim), shape_of(BF16, 2, j_n, dim, dim),
            shape_of(F32, n_c, 2, j_n, 1, cols), shape_of(F32, 2, e, 1), shape_of(F32, n_b, dim, s_len),
        ],
        scratch_shapes=[
            pltpu.VMEM((n_b, dim, s_len), F32),
            pltpu.VMEM((2 * dim, dim), F32),
            pltpu.VMEM((2 * rows, s_len), BF16),
            pltpu.VMEM((2 * cols, s_len), BF16), pltpu.VMEM((2 * rows, s_len), BF16),
            pltpu.VMEM((2 * cols, s_len), BF16), pltpu.VMEM((2 * rows, s_len), BF16),
            pltpu.VMEM((dim, 2 * cols), BF16),
        ],
        compiler_params=params(1),
        cost_estimate=pl.CostEstimate(flops=4 * heads * s_len * (dim * dim + 10 * s_len * e), bytes_accessed=10 ** 7, transcendentals=heads * s_len * s_len),
        name="block_bwd",
    )(d_br, h_t, *ws, qk, cos_t, sin_t, y, o, lse)


def even_first(arr, e):
    lead = arr.shape[:-1]
    return jnp.swapaxes(arr.reshape(*lead, e // 2, 2), -1, -2).reshape(*lead, e)


def interleave(arr, e):
    lead = arr.shape[:-1]
    return jnp.swapaxes(arr.reshape(*lead, 2, e // 2), -1, -2).reshape(*lead, e)


def solution(mesh):
    n_tp = mesh.shape["tp"]
    act, part, heads1, heads2, whole = P("dp", "tp"), P("dp"), P(None, "tp"), P(None, None, "tp"), P()
    in_specs = (act, part, P("tp"), P("tp"), whole, whole, heads2, heads1, whole, whole, heads1, whole, act)
    out_specs = (act, act, part, part, P("dp", None, "tp"), act, part, part, act, part)
    peer_core = [(i, i ^ 1) for i in range(n_tp)]
    across = [(i, i ^ 2) for i in range(n_tp)]

    def swap(arr):
        return lax.all_to_all(arr, "tp", 0, 0)

    def device_step(x_in, cond_vec, rope_cos, rope_sin, w_mod, b_mod, w_in, b_in, q_scale, k_scale, w_out, b_out, d_out):
        n_l, dim, n_j, cols = w_in.shape
        e = q_scale.shape[1]
        n_all, s_own = x_in.shape[:2]
        n_b = n_all // n_tp
        me = lax.axis_index("tp")
        pairs = np.arange(e).reshape(e // 2, 2).T.reshape(-1)
        perm = np.concatenate([pairs, e + pairs, np.arange(2 * e, cols)])
        perm_mat = jnp.asarray(np.eye(cols, dtype=np.float32)[perm], BF16)

        n_rope = e * s_own
        b_perm = jnp.einsum("ec,lhc->lhe", perm_mat, b_in, preferred_element_type=F32)
        small_in = jnp.concatenate([rope_cos.T.reshape(-1), rope_sin.T.reshape(-1), b_perm.reshape(-1)])
        small_all = lax.all_gather(small_in, "tp", axis=0, tiled=False)
        tie = swap(x_in.reshape(n_tp, n_b, s_own, dim))
        w_local = []
        for l in range(n_l):
            w_in_t = jnp.einsum("ec,dhc->hed", perm_mat, w_in[l], preferred_element_type=F32).astype(BF16)
            w_local.append(jnp.concatenate([w_in_t, w_out[l]], axis=1))
        w_own = [(w, lax.ppermute(w, "tp", peer_core)) for w in w_local]

        tables = jnp.moveaxis(small_all[:, :n_rope].reshape(n_tp, e, s_own), 0, 1).reshape(e, n_tp * s_own)
        cos_t, sin_t = tables[:e // 2], tables[e // 2:]
        b_all = small_all[:, n_rope:].reshape(n_tp, n_l, n_j, 1, cols)
        b_rel = jnp.stack([lax.dynamic_index_in_dim(b_all, me ^ i, 0, keepdims=False) for i in range(n_tp)])
        b_rel = jnp.broadcast_to(b_rel, (n_tp, n_l, n_j, 8, cols))

        silu_all = jax.nn.silu(cond_vec.astype(F32)).astype(BF16)
        silu_own = lax.dynamic_slice_in_dim(silu_all, me * n_b, n_b, 0)
        mod = jnp.einsum("bd,ldm->lbm", silu_own, w_mod, preferred_element_type=F32) + b_mod.astype(F32)[:, None]
        bias = jnp.broadcast_to(b_out.astype(F32)[:, None, None], (n_l, n_b, 5, dim))
        mod_rows = jnp.concatenate([mod.reshape(n_l, n_b, 3, dim), bias], axis=2)
        qk = even_first(jnp.stack([q_scale, k_scale], axis=1).astype(F32), e)
        qk = jnp.broadcast_to(qk[:, :, None], (n_l, 2, 8, e))

        saved, ws = [], []
        for l in range(n_l):
            consts = (qk[l], cos_t, sin_t)
            mine, tie = lax.optimization_barrier((w_local[l], tie))
            if l == 0:
                x_cur = tie
            got = lax.ppermute(mine, "tp", across)
            half = block_forward(0, x_cur, mod_rows[l], w_own[l], b_rel[:2, l], *consts, (), l == 0, 0)
            x_t = half[4] if l == 0 else x_cur
            got, h_t = lax.optimization_barrier((got, half[3]))
            tie = got
            w_other = (got, lax.ppermute(got, "tp", peer_core))
            y, o, lse, branch, x_cur = block_forward(1, x_t, mod_rows[l], w_other, b_rel[2:, l], *consts, (*half[:3], h_t, half[-1]), False, n_tp * (l == n_l - 1))
            saved.append((x_t, y, o, lse, h_t, branch))
            ws.append((*w_own[l], *w_other))
        d_late, tie = lax.optimization_barrier((d_out, tie))
        g_tok = swap(d_late.reshape(n_tp, n_b, s_own, dim))
        x_out = swap(x_cur)

        grads, small = [None] * n_l, [None] * n_l
        top = n_l - 1
        g_t, d_br, sums_in = edge(g_tok, (), (mod_rows[top], saved[top][5]), True, 0)
        d_gate, d_bias = sums_in[:, 0], sums_in[:, 1]
        for l in reversed(range(n_l)):
            x_t, y, o, lse, h_t, branch = saved[l]
            if l == 0:
                d_br, x_out = lax.optimization_barrier((d_br, x_out))
            d_hs, d_qk, gb, gw = [], 0.0, [], []
            for j, width in ((0, n_j),) if l else ((0, n_j - 1), (n_j - 1, 1)):
                keep, send, gb_j, dqk_j, dh_j = block_backward(j, width, d_br, h_t, ws[l], qk[l], cos_t, sin_t, y, o, lse)
                d_hs.append(dh_j)
                d_qk = d_qk + dqk_j
                gb.append(gb_j)
                near = lax.ppermute(send, "tp", peer_core)
                leaving = (keep[1].astype(F32) + near[1].astype(F32)).astype(BF16)
                far = lax.ppermute(leaving, "tp", across)
                gw.append((keep[0].astype(F32) + near[0].astype(F32) + far.astype(F32)).astype(BF16))
            entry = (mod_rows[l - 1], saved[l - 1][5]) if l > 0 else ()
            edge_out = edge(g_t, (x_t, mod_rows[l], d_hs), entry, False, n_tp * (l == 0))
            g_t, sums = edge_out[0], edge_out[-1]
            grads[l] = jnp.concatenate(gw)
            d_mod = jnp.stack([sums[:, 0], sums[:, 1], d_gate], axis=1)
            gb = jnp.concatenate(gb, axis=2).reshape(2, 2, n_j * cols)
            gb = jnp.stack([lax.dynamic_index_in_dim(lax.dynamic_index_in_dim(gb, (i ^ me) % 2, 0, keepdims=False), (i ^ me) // 2, 0, keepdims=False) for i in range(n_tp)])
            small[l] = jnp.concatenate([d_mod.reshape(-1), jnp.sum(d_bias, axis=0), d_qk.reshape(-1), gb.reshape(-1)])
            if l > 0:
                d_br = edge_out[1]
                d_gate, d_bias = sums[:, 2], sums[:, 3]

        gathered = swap(jnp.broadcast_to(jnp.stack(small), (n_tp, n_l, small[0].shape[0])))
        grad_x = swap(g_t)
        n_mod = n_b * 3 * dim
        d_mod = jnp.moveaxis(gathered[:, :, :n_mod].reshape(n_tp, n_l, n_b, 3 * dim), 1, 0).reshape(n_l, n_all, 3 * dim)
        sums = jnp.sum(gathered[:, :, n_mod:], axis=0)
        g_wmod = wmod_grad(silu_all, d_mod)
        g_bmod = jnp.sum(d_mod, axis=1)
        g_qk = interleave(sums[:, dim:dim + 2 * e].reshape(n_l, 2, e), e)
        g_b = lax.dynamic_index_in_dim(sums[:, dim + 2 * e:].reshape(n_l, n_tp, n_j, cols), me, 1, keepdims=False)
        g_bin = jnp.concatenate([interleave(g_b[..., :e], e), interleave(g_b[..., e:2 * e], e), g_b[..., 2 * e:]], axis=-1)
        gw_all = jnp.stack(grads)
        g_win = jnp.einsum("ec,lhed->ldhc", perm_mat, gw_all[:, :, :cols], preferred_element_type=F32).astype(BF16)
        return (x_out.reshape(n_all, s_own, dim), grad_x.reshape(n_all, s_own, dim), g_wmod, g_bmod, g_win, g_bin, g_qk[:, 0], g_qk[:, 1], gw_all[:, :, cols:], sums[:, :dim])

    return jax.shard_map(device_step, mesh=mesh, in_specs=in_specs, out_specs=out_specs, check_vma=False)
```

```python
import functools
import jax
import jax.numpy as jnp
import numpy as np
from jax import lax
from jax.experimental import pallas as pl
from jax.experimental.pallas import tpu as pltpu
from jax.sharding import PartitionSpec as P

NORM_EPS = 1e-6
LOG2E = 1.4426950408889634
GELU_C = 0.7978845608028654
GELU_A = 0.044715
F32 = jnp.float32
BF16 = jnp.bfloat16
CHUNK = 512
VMEM = 63 * 1024 * 1024
SPLIT = 2
SQ = pl.squeezed
FULL = ...


def dot_nn(a, b):
    return lax.dot_general(a, b, (((1,), (0,)), ((), ())), preferred_element_type=F32)


def dot_nt(a, b):
    return lax.dot_general(a, b, (((1,), (1,)), ((), ())), preferred_element_type=F32)


def dot_tn(a, b):
    return lax.dot_general(a, b, (((0,), (0,)), ((), ())), preferred_element_type=F32)


def norm_rope(raw, scale_col, cos_t, sin_t):
    half = raw.shape[0] // 2
    inv = lax.rsqrt(jnp.mean(raw * raw, axis=0, keepdims=True) + NORM_EPS)
    hat = raw * inv
    scaled = hat * scale_col
    a, b = scaled[:half], scaled[half:]
    rot = jnp.concatenate([a * cos_t - b * sin_t, a * sin_t + b * cos_t], axis=0)
    return hat, inv, rot.astype(BF16)


def norm_rope_bwd(d_rot, hat, inv, scale_col, cos_t, sin_t):
    half = d_rot.shape[0] // 2
    da, db = d_rot[:half], d_rot[half:]
    d_scaled = jnp.concatenate([da * cos_t + db * sin_t, db * cos_t - da * sin_t], axis=0)
    d_scale = jnp.sum(d_scaled * hat, axis=1, keepdims=True)
    d_hat = d_scaled * scale_col
    d_raw = inv * (d_hat - hat * jnp.mean(d_hat * hat, axis=0, keepdims=True))
    return d_raw, d_scale


def softmax_head(q_rot, k_rot, v_t, o_ref, lse_ref, i, mul, between):
    n_c = q_rot.shape[1] // CHUNK
    spans = [slice(c * CHUNK, (c + 1) * CHUNK) for c in range(n_c)]
    nxt = dot_tn(k_rot, q_rot[:, spans[0]])
    outs = []
    for c in range(n_c):
        s = nxt
        if c + 1 < n_c:
            nxt = dot_tn(k_rot, q_rot[:, spans[c + 1]])
        between(c, outs)
        top = jnp.max(s, axis=0, keepdims=True) * mul
        p = jnp.exp2(s * mul - top)
        tot = jnp.sum(p, axis=0, keepdims=True)
        out = (dot_nn(v_t, p.astype(BF16)) * (1.0 / tot)).astype(BF16)
        o_ref[i, :, spans[c]] = out
        outs.append(out)
        lse_ref[i:i + 1, spans[c]] = top + jnp.log2(tot)
    return jnp.concatenate(outs, axis=1)


def as_col(rows):
    return rows.T


def as_row(col):
    n = col.shape[0]
    return jnp.broadcast_to(col, (n, 128)).T[:1]


def from_tokens(ref):
    return jnp.concatenate([ref[t].astype(F32).T for t in range(ref.shape[0])], axis=1)


def gelu_parts(u):
    t = jnp.tanh(GELU_C * (u + GELU_A * u * u * u))
    return t, 0.5 * (1.0 + t)


def fwd_kernel(e, first, last, token_in, token_out, *refs):
    refs = list(refs)
    take = refs.pop
    mod_ref, wa_ref, wb_ref, bin_ref, qk_ref, cos_ref, sin_ref, x_ref = [take(0) for _ in range(8)]
    if not first:
        h_in, z_in = take(0), take(0)
        del refs[:3]
    y_ref, o_ref, lse_ref = take(0), take(0), take(0)
    if first:
        h_ref = take(0)
        if token_in:
            xt_ref = take(0)
    if last:
        br_ref = take(0)
        xo_ref = take(0)
    else:
        z_out = take(0)
    z_sc, h_sc, wo_sc = refs
    g, b = pl.program_id(0), pl.program_id(1)
    final = pl.num_programs(0) - 1
    cols = bin_ref.shape[-1]

    @pl.when(g == 0)
    def _():
        if first:
            mod = as_col(mod_ref[FULL])
            if token_in:
                x = from_tokens(x_ref)
                xt_ref[FULL] = x.astype(BF16)
            else:
                x = x_ref[FULL].astype(F32)
            cent = x - jnp.mean(x, axis=0, keepdims=True)
            normed = cent * lax.rsqrt(jnp.mean(cent * cent, axis=0, keepdims=True) + NORM_EPS)
            h = (normed * (1.0 + mod[:, 1:2]) + mod[:, :1]).astype(BF16)
            h_sc[b] = h
            h_ref[FULL] = h
            z_sc[b] = jnp.zeros_like(x)
        else:
            h_sc[b] = h_in[FULL]
            z_sc[b] = z_in[FULL]

    h_t = h_sc[b]
    cos_t, sin_t = cos_ref[FULL], sin_ref[FULL]
    q_col, k_col = [as_col(qk_ref[i])[:, :1] for i in range(2)]
    mul = (e ** -0.5) * LOG2E
    n_c = h_t.shape[1] // CHUNK
    spans = [slice(c * CHUNK, (c + 1) * CHUNK) for c in range(n_c)]
    bias = [as_col(bin_ref[i])[:, :1] for i in range(2)]
    wo_sc[FULL] = jnp.concatenate([wa_ref[cols:], wb_ref[cols:]], axis=0).T
    y_a = dot_nn(wa_ref[:cols], h_t) + bias[0]
    y_ref[0] = y_a

    def next_head(c, outs):
        y_ref[1, :, spans[c]] = dot_nn(wb_ref[:cols], h_t[:, spans[c]]) + bias[1]

    def attend(i, y, between):
        q_rot = norm_rope(y[:e], q_col, cos_t, sin_t)[-1]
        k_rot = norm_rope(y[e:2 * e], k_col, cos_t, sin_t)[-1]
        return softmax_head(q_rot, k_rot, y[2 * e:3 * e].astype(BF16), o_ref, lse_ref, i, mul, between)

    def mlp(u):
        return (u * gelu_parts(u)[1]).astype(BF16)

    def project(c, outs):
        tall = jnp.concatenate([o_a[:, spans[c]], m_a[:, spans[c]], outs[c], m_b[:, spans[c]]], axis=0)
        z_sc[b, :, spans[c]] += dot_nn(wo_sc[FULL], tall)

    def project_late(c, outs):
        if c > 0:
            project(c - 1, outs)

    o_a = attend(0, y_a, next_head)
    m_a = mlp(y_a[3 * e:])
    m_b = mlp(y_ref[1, 3 * e:])
    o_b = attend(1, y_ref[1, :3 * e], project_late)
    project(n_c - 1, [o_b[:, span] for span in spans])

    @pl.when(g == final)
    def _():
        if last:
            mod = as_col(mod_ref[FULL])
            branch = z_sc[b] + mod[:, 3:4]
            br_ref[FULL] = branch
            x_new = x_ref[FULL].astype(F32) + mod[:, 2:3] * branch
            if token_out:
                s_t = xo_ref.shape[1]
                for t in range(token_out):
                    xo_ref[t] = x_new[:, t * s_t:(t + 1) * s_t].T.astype(BF16)
            else:
                xo_ref[FULL] = x_new.astype(BF16)
        else:
            z_out[FULL] = z_sc[b]


def bwd_kernel(e, dbr_ref, h_ref, wa0_ref, wb0_ref, wa1_ref, wb1_ref, qk_ref, cos_ref, sin_ref, y_ref, o_ref, lse_ref, keep_ref, send_ref, gb_ref, dqk_ref, dh_ref, dh_sc, acc_sc, dj_sc, dp_new, jn_new, dp_sc, jn_sc, win_sc):
    step = pl.program_id(0)
    n = pl.num_programs(0) - 1
    cols = y_ref.shape[1]
    rows = dj_sc.shape[0] // 2
    s_len = dbr_ref.shape[-1]
    b = lax.rem(step, 2)
    scale = e ** -0.5
    mul = scale * LOG2E

    @pl.when(step == 0)
    def _():
        for ref in (dqk_ref, dh_sc, acc_sc, dp_sc, jn_sc, win_sc):
            ref[FULL] = jnp.zeros_like(ref)

    def dense():
        b_prev = 1 - b
        again = b_prev.astype(F32)
        gwi = dot_nt(dp_sc[FULL], h_ref[b_prev]) + again * acc_sc[:2 * cols]
        acc_sc[:2 * cols] = gwi
        gwo = dot_nt(jn_sc[FULL], dbr_ref[b_prev]) + again * acc_sc[2 * cols:]
        acc_sc[2 * cols:] = gwo
        for i, ref in enumerate((keep_ref, send_ref)):
            ref[:cols] = gwi[i * cols:(i + 1) * cols].astype(BF16)
            ref[cols:] = gwo[i * rows:(i + 1) * rows].astype(BF16)
        dh_sc[b_prev] += dot_nn(win_sc[FULL], dp_sc[FULL])

    def attention():
        own = lax.rem(step // 2, 2) == 0
        d_br = dbr_ref[b]
        cos_t, sin_t = cos_ref[FULL], sin_ref[FULL]
        q_col, k_col = [as_col(qk_ref[i])[:, :1] for i in range(2)]
        w_pair = [jnp.where(own, x[FULL], y[FULL]) for x, y in ((wa0_ref, wa1_ref), (wb0_ref, wb1_ref))]
        for i in range(2):
            dj_sc[i * rows:(i + 1) * rows] = dot_nn(w_pair[i][cols:], d_br).astype(BF16)
        sums = []
        for i in range(2):
            q_hat, q_inv, q_rot = norm_rope(y_ref[i, :e], q_col, cos_t, sin_t)
            k_hat, k_inv, k_rot = norm_rope(y_ref[i, e:2 * e], k_col, cos_t, sin_t)
            v_t = y_ref[i, 2 * e:3 * e].astype(BF16)
            o_t = o_ref[i]
            d_o = dj_sc[i * rows:i * rows + e]
            d_sum = jnp.sum(d_o.astype(F32) * o_t.astype(F32), axis=0, keepdims=True)
            d_q, d_k, d_v = [], 0.0, 0.0
            for c in range(s_len // CHUNK):
                span = slice(c * CHUNK, (c + 1) * CHUNK)
                p = jnp.exp2(dot_tn(k_rot, q_rot[:, span]) * mul - lse_ref[i:i + 1, span])
                d_p = dot_tn(v_t, d_o[:, span])
                d_s = (p * (d_p - d_sum[:, span])).astype(BF16)
                d_q.append(dot_nn(k_rot, d_s))
                d_k = d_k + dot_nt(q_rot[:, span], d_s)
                d_v = d_v + dot_nt(d_o[:, span], p.astype(BF16))
            d_qraw, d_qs = norm_rope_bwd(jnp.concatenate(d_q, axis=1) * scale, q_hat, q_inv, q_col, cos_t, sin_t)
            d_kraw, d_ks = norm_rope_bwd(d_k * scale, k_hat, k_inv, k_col, cos_t, sin_t)
            dqk_ref[0] += d_qs
            dqk_ref[1] += d_ks
            u = y_ref[i, 3 * e:]
            t, half = gelu_parts(u)
            jn_new[i * rows:i * rows + e] = o_t
            jn_new[i * rows + e:(i + 1) * rows] = (u * half).astype(BF16)
            slope = half + 0.5 * u * (1.0 - t * t) * (GELU_C * (1.0 + 3.0 * GELU_A * u * u))
            d_u = dj_sc[i * rows + e:(i + 1) * rows].astype(F32) * slope
            off = i * cols
            part_sums = []
            for part in (d_qraw, d_kraw, d_v, d_u):
                dp_new[off:off + part.shape[0]] = part.astype(BF16)
                part_sums.append(jnp.sum(part, axis=1, keepdims=True))
                off += part.shape[0]
            sums.append(as_row(jnp.concatenate(part_sums, axis=0)))
        for i in range(2):
            gb_ref[i] = jnp.where(b == 0, sums[i], gb_ref[i] + sums[i])
        return w_pair

    @pl.when(step < n)
    def _():
        dense()
        w_pair = attention()
        dp_sc[FULL] = dp_new[FULL]
        jn_sc[FULL] = jn_new[FULL]
        win_sc[FULL] = jnp.concatenate([w[:cols] for w in w_pair], axis=0).T

    @pl.when(step == n)
    def _():
        dense()

    @pl.when(step >= n - 1)
    def _():
        dh_ref[FULL] = dh_sc[1 - b]


def edge_kernel(n_exit, has_entry, token_g, token_out, *refs):
    refs = list(refs)
    take = refs.pop
    g_ref = take(0)
    if n_exit:
        x_ref, mod_ref = take(0), take(0)
        dh_refs = [take(0) for _ in range(n_exit)]
    if has_entry:
        mod2_ref, br_ref = take(0), take(0)
    if n_exit:
        gx_ref = take(0)
    if has_entry:
        if token_g:
            gt_ref = take(0)
        dbr_ref = take(0)
    sum_ref = take(0)
    grad = from_tokens(g_ref) if token_g else g_ref[FULL].astype(F32)
    parts = []
    if n_exit:
        d_h = dh_refs[0][FULL]
        for ref in dh_refs[1:]:
            d_h = d_h + ref[FULL]
        x = x_ref[FULL].astype(F32)
        cent = x - jnp.mean(x, axis=0, keepdims=True)
        inv = lax.rsqrt(jnp.mean(cent * cent, axis=0, keepdims=True) + NORM_EPS)
        hat = cent * inv
        parts += [jnp.sum(d_h, axis=1, keepdims=True), jnp.sum(d_h * hat, axis=1, keepdims=True)]
        d_hat = d_h * (1.0 + as_col(mod_ref[FULL])[:, 1:2])
        d_x = inv * (d_hat - jnp.mean(d_hat, axis=0, keepdims=True) - hat * jnp.mean(d_hat * hat, axis=0, keepdims=True))
        grad = grad + d_x
        if token_out:
            s_t = gx_ref.shape[1]
            for t in range(gx_ref.shape[0]):
                gx_ref[t] = grad[:, t * s_t:(t + 1) * s_t].T.astype(BF16)
        else:
            gx_ref[FULL] = grad.astype(BF16)
            grad = grad.astype(BF16).astype(F32)
    if has_entry:
        if token_g:
            gt_ref[FULL] = grad.astype(BF16)
        gated = grad * as_col(mod2_ref[FULL])[:, 2:3]
        parts += [jnp.sum(grad * br_ref[FULL], axis=1, keepdims=True), jnp.sum(gated, axis=1, keepdims=True)]
        dbr_ref[FULL] = gated.astype(BF16)

    @pl.when(pl.program_id(1) == 0)
    def _():
        sum_ref[FULL] = jnp.zeros_like(sum_ref)

    for i, part in enumerate(parts):
        sum_ref[i:i + 1] += as_row(part)


def params(n_axes):
    return pltpu.CompilerParams(dimension_semantics=("arbitrary",) * n_axes, vmem_limit_bytes=VMEM)


def shape_of(dtype, *shape):
    return jax.ShapeDtypeStruct(shape, dtype)


def edge(grad, exit_args, entry_args, token_g, token_out):
    if token_g:
        n_t, n_b, s_t, dim = grad.shape
    else:
        n_t, (n_b, dim, s_t) = token_out or SPLIT, grad.shape
        s_t = s_t // n_t
    act = pl.BlockSpec((SQ, dim, n_t * s_t // SPLIT), lambda b, t: (b, 0, t))
    rows = pl.BlockSpec((SQ, 8, dim), lambda b, t: (b, 0, 0))
    tok = pl.BlockSpec((n_t // SPLIT, SQ, s_t, dim), lambda b, t: (t, b, 0, 0))
    shape_act = shape_of(BF16, n_b, dim, n_t * s_t)
    args, in_specs, out_specs, out_shape = [grad], [tok if token_g else act], [], []
    if exit_args:
        x_t, mod_l, d_hs = exit_args
        args += [x_t, mod_l, *d_hs]
        in_specs += [act, rows] + [act] * len(d_hs)
        out_specs.append(tok if token_out else act)
        out_shape.append(shape_of(BF16, n_t, n_b, s_t, dim) if token_out else shape_act)
    if entry_args:
        args += entry_args
        in_specs += [rows, act]
        out_specs += [act] * (1 + token_g)
        out_shape += [shape_act] * (1 + token_g)
    return pl.pallas_call(
        functools.partial(edge_kernel, len(exit_args[2]) if exit_args else 0, bool(entry_args), token_g, token_out),
        grid=(n_b, SPLIT), in_specs=in_specs, out_specs=out_specs + [rows], out_shape=out_shape + [shape_of(F32, n_b, 8, dim)],
        compiler_params=params(2),
        cost_estimate=pl.CostEstimate(flops=10 ** 6, bytes_accessed=10 ** 7, transcendentals=0),
        name="edge",
    )(*args)


def wmod_kernel(s_ref, d_ref, o_ref):
    o_ref[FULL] = dot_tn(s_ref[FULL], d_ref[FULL].astype(BF16))


def wmod_grad(silu_all, d_mod):
    n_l, n_all, width = d_mod.shape
    dim = silu_all.shape[1]
    piece = dim // 3
    return pl.pallas_call(
        wmod_kernel,
        grid=(n_l, 3),
        in_specs=[pl.BlockSpec((n_all, piece), lambda l, i: (0, i)), pl.BlockSpec((SQ, n_all, width), lambda l, i: (l, 0, 0))],
        out_specs=pl.BlockSpec((SQ, piece, width), lambda l, i: (l, i, 0)),
        out_shape=shape_of(F32, n_l, dim, width),
        compiler_params=params(2),
        cost_estimate=pl.CostEstimate(flops=10 ** 6, bytes_accessed=10 ** 7, transcendentals=0),
        name="wmod_grad",
    )(silu_all, d_mod)


def block_forward(slot, j_lo, last, x_in, mod_rows, w_pair, b_rows, qk, cos_t, sin_t, prev, token_in, token_out):
    first = slot == 0
    token_in = token_in and first
    j_n, dim = w_pair[0].shape[:2]
    n_c, n_j = b_rows.shape[:2]
    cols = b_rows.shape[-1]
    e = qk.shape[-1]
    s_len = cos_t.shape[1]
    n_b = mod_rows.shape[0]
    final = j_n - 1
    full = lambda *shape: pl.BlockSpec(shape, lambda g, b: (0,) * len(shape))
    head6 = lambda n, m: pl.BlockSpec((SQ, SQ, n_c, SQ, n, m), lambda g, b: (b, slot, 0, j_lo + g, 0, 0))
    act = lambda idx: pl.BlockSpec((SQ, dim, s_len), lambda g, b: (idx(g, b), 0, 0))
    at_start = lambda g, b: jnp.where(g == 0, b, n_b - 1)
    at_end = lambda g, b: jnp.where(g == final, b, 0)
    tok = lambda n, idx: pl.BlockSpec((n, SQ, s_len // n, dim), lambda g, b: (0, idx(g, b), 0, 0))
    weight = pl.BlockSpec((SQ, dim, dim), lambda g, b: (g, 0, 0))
    args = [mod_rows, *w_pair, b_rows, qk, cos_t, sin_t, x_in]
    in_specs = [
        pl.BlockSpec((SQ, 8, dim), lambda g, b: (b, 0, 0)), weight, weight,
        pl.BlockSpec((n_c, SQ, 8, cols), lambda g, b: (0, j_lo + g, 0, 0)),
        full(2, 8, e), full(e // 2, s_len), full(e // 2, s_len),
        tok(x_in.shape[0], at_start) if token_in else act(at_start if first else at_end),
    ]
    aliases = {}
    if not first:
        args += [prev[3], prev[4], *prev[:3]]
        in_specs += [act(at_start), act(at_start)] + [pl.BlockSpec(memory_space=pl.ANY)] * 3
        aliases = {len(args) - 3 + i: i for i in range(3)}
    shape16, shape32 = shape_of(BF16, n_b, dim, s_len), shape_of(F32, n_b, dim, s_len)
    out_specs = [head6(cols, s_len), head6(e, s_len), pl.BlockSpec((SQ, SQ, SQ, n_c, s_len), lambda g, b: (b, slot, j_lo + g, 0, 0))]
    out_shape = [shape_of(F32, n_b, 2, n_c, n_j, cols, s_len), shape_of(BF16, n_b, 2, n_c, n_j, e, s_len), shape_of(F32, n_b, 2, n_j, n_c, s_len)]
    if first:
        out_specs += [act(at_start)] * (1 + token_in)
        out_shape += [shape16] * (1 + token_in)
    out_specs.append(act(at_end))
    out_shape.append(shape32)
    if last:
        out_specs.append(tok(token_out, at_end) if token_out else act(at_end))
        out_shape.append(shape_of(BF16, token_out, n_b, s_len // token_out, dim) if token_out else shape16)
    heads = n_c * j_n * n_b
    return pl.pallas_call(
        functools.partial(fwd_kernel, e, first, last, token_in, token_out),
        grid=(j_n, n_b), in_specs=in_specs, out_specs=out_specs, out_shape=out_shape,
        input_output_aliases=aliases,
        scratch_shapes=[pltpu.VMEM((n_b, dim, s_len), F32), pltpu.VMEM((n_b, dim, s_len), BF16), pltpu.VMEM((dim, 2 * (dim - cols)), BF16)],
        compiler_params=params(2),
        cost_estimate=pl.CostEstimate(flops=2 * heads * s_len * (dim * dim + 8 * s_len * e), bytes_accessed=10 ** 7, transcendentals=heads * s_len * s_len),
        name="block_fwd",
    )(*args)


def block_backward(j_lo, j_n, d_br, h_t, ws, qk, cos_t, sin_t, y, o, lse):
    n_b, dim, s_len = d_br.shape
    n_c, cols = y.shape[2], y.shape[4]
    e = qk.shape[-1]
    rows = dim - cols
    n = 2 * j_n * n_b
    group = lambda s: jnp.minimum(s, n - 1) // n_b
    before = lambda s: jnp.maximum(s - 1, 0) // n_b
    once = pl.Buffered(1)
    full = lambda *shape: pl.BlockSpec(shape, lambda s: (0,) * len(shape), pipeline_mode=once)
    head6 = lambda n_r, m: pl.BlockSpec((SQ, SQ, n_c, SQ, n_r, m), lambda s: (jnp.minimum(s, n - 1) % n_b, group(s) % 2, 0, j_lo + group(s) // 2, 0, 0))

    def weight(w):
        base = 0 if w.shape[0] == j_n else j_lo
        return pl.BlockSpec((SQ, dim, dim), lambda s: (base + group(s) // 2, 0, 0))

    grad = pl.BlockSpec((SQ, SQ, dim, dim), lambda s: (before(s) % 2, before(s) // 2, 0, 0))
    heads = 2 * n_c * j_n * n_b
    return pl.pallas_call(
        functools.partial(bwd_kernel, e),
        grid=(n + 1,),
        in_specs=[
            full(n_b, dim, s_len), full(n_b, dim, s_len), *[weight(w) for w in ws],
            full(2, 8, e), full(e // 2, s_len), full(e // 2, s_len),
            head6(cols, s_len), head6(e, s_len),
            pl.BlockSpec((SQ, SQ, SQ, n_c, s_len), lambda s: (jnp.minimum(s, n - 1) % n_b, group(s) % 2, j_lo + group(s) // 2, 0, 0)),
        ],
        out_specs=[
            grad, grad,
            pl.BlockSpec((n_c, SQ, SQ, 1, cols), lambda s: (0, group(s) % 2, group(s) // 2, 0, 0)),
            pl.BlockSpec((2, e, 1), lambda s: (0, 0, 0)),
            pl.BlockSpec((SQ, dim, s_len), lambda s: (jnp.where(s == n, 1, 0), 0, 0)),
        ],
        out_shape=[
            shape_of(BF16, 2, j_n, dim, dim), shape_of(BF16, 2, j_n, dim, dim),
            shape_of(F32, n_c, 2, j_n, 1, cols), shape_of(F32, 2, e, 1), shape_of(F32, n_b, dim, s_len),
        ],
        scratch_shapes=[
            pltpu.VMEM((n_b, dim, s_len), F32),
            pltpu.VMEM((2 * dim, dim), F32),
            pltpu.VMEM((2 * rows, s_len), BF16),
            pltpu.VMEM((2 * cols, s_len), BF16), pltpu.VMEM((2 * rows, s_len), BF16),
            pltpu.VMEM((2 * cols, s_len), BF16), pltpu.VMEM((2 * rows, s_len), BF16),
            pltpu.VMEM((dim, 2 * cols), BF16),
        ],
        compiler_params=params(1),
        cost_estimate=pl.CostEstimate(flops=4 * heads * s_len * (dim * dim + 10 * s_len * e), bytes_accessed=10 ** 7, transcendentals=heads * s_len * s_len),
        name="block_bwd",
    )(d_br, h_t, *ws, qk, cos_t, sin_t, y, o, lse)


def even_first(arr, e):
    lead = arr.shape[:-1]
    return jnp.swapaxes(arr.reshape(*lead, e // 2, 2), -1, -2).reshape(*lead, e)


def interleave(arr, e):
    lead = arr.shape[:-1]
    return jnp.swapaxes(arr.reshape(*lead, 2, e // 2), -1, -2).reshape(*lead, e)


def solution(mesh):
    n_tp = mesh.shape["tp"]
    act, part, heads1, heads2, whole = P("dp", "tp"), P("dp"), P(None, "tp"), P(None, None, "tp"), P()
    in_specs = (act, part, P("tp"), P("tp"), whole, whole, heads2, heads1, whole, whole, heads1, whole, act)
    out_specs = (act, act, part, part, P("dp", None, "tp"), act, part, part, act, part)
    peer_core = [(i, i ^ 1) for i in range(n_tp)]
    across = [(i, i ^ 2) for i in range(n_tp)]

    def swap(arr):
        return lax.all_to_all(arr, "tp", 0, 0)

    def device_step(x_in, cond_vec, rope_cos, rope_sin, w_mod, b_mod, w_in, b_in, q_scale, k_scale, w_out, b_out, d_out):
        n_l, dim, n_j, cols = w_in.shape
        e = q_scale.shape[1]
        n_all, s_own = x_in.shape[:2]
        n_b = n_all // n_tp
        me = lax.axis_index("tp")
        pairs = np.arange(e).reshape(e // 2, 2).T.reshape(-1)
        perm = np.concatenate([pairs, e + pairs, np.arange(2 * e, cols)])
        perm_mat = jnp.asarray(np.eye(cols, dtype=np.float32)[perm], BF16)

        n_rope = e * s_own
        b_perm = jnp.einsum("ec,lhc->lhe", perm_mat, b_in, preferred_element_type=F32)
        small_in = jnp.concatenate([rope_cos.T.reshape(-1), rope_sin.T.reshape(-1), b_perm.reshape(-1)])
        silu_all = jax.nn.silu(cond_vec.astype(F32)).astype(BF16)
        silu_own = lax.dynamic_slice_in_dim(silu_all, me * n_b, n_b, 0)
        mod_sum = jnp.einsum("bd,ldm->lbm", silu_own, w_mod, preferred_element_type=F32)
        mod = mod_sum + b_mod.astype(F32)[:, None]
        bias = jnp.broadcast_to(b_out.astype(F32)[:, None, None], (n_l, n_b, 5, dim))
        mod_rows = jnp.concatenate([mod.reshape(n_l, n_b, 3, dim), bias], axis=2)
        small_in, mod_rows = lax.optimization_barrier((small_in, mod_rows))
        small_all = lax.all_gather(small_in, "tp", axis=0, tiled=False)
        tie = swap(x_in.reshape(n_tp, n_b, s_own, dim))
        w_local = []
        for l in range(n_l):
            w_in_t = jnp.einsum("ec,dhc->hed", perm_mat, w_in[l], preferred_element_type=F32).astype(BF16)
            w_local.append(jnp.concatenate([w_in_t, w_out[l]], axis=1))
        w_own = [(w, lax.ppermute(w, "tp", peer_core)) for w in w_local]

        tables = jnp.moveaxis(small_all[:, :n_rope].reshape(n_tp, e, s_own), 0, 1).reshape(e, n_tp * s_own)
        cos_t, sin_t = tables[:e // 2], tables[e // 2:]
        b_all = small_all[:, n_rope:].reshape(n_tp, n_l, n_j, 1, cols)
        b_rel = jnp.stack([lax.dynamic_index_in_dim(b_all, me ^ i, 0, keepdims=False) for i in range(n_tp)])
        b_rel = jnp.broadcast_to(b_rel, (n_tp, n_l, n_j, 8, cols))

        qk = even_first(jnp.stack([q_scale, k_scale], axis=1).astype(F32), e)
        qk = jnp.broadcast_to(qk[:, :, None], (n_l, 2, 8, e))

        saved, ws = [], []
        for l in range(n_l):
            consts = (qk[l], cos_t, sin_t)
            mine, tie = lax.optimization_barrier((w_local[l], tie))
            if l == 0:
                x_cur = tie
            cuts = (0, n_j - 1, n_j) if l == 0 else (0, n_j)
            bounds = list(zip(cuts[:-1], cuts[1:]))
            arriving = [lax.ppermute(mine[lo:hi], "tp", across) for lo, hi in bounds]
            half = block_forward(0, 0, False, x_cur, mod_rows[l], w_own[l], b_rel[:2, l], *consts, (), l == 0, 0)
            x_t = half[4] if l == 0 else x_cur
            y, o, lse, h_t = half[:4]
            z = half[-1]
            others = []
            for got, (lo, hi) in zip(arriving, bounds):
                end = hi == n_j
                got, z = lax.optimization_barrier((got, z))
                tie = got
                others.append((lo, hi - lo, (got, lax.ppermute(got, "tp", peer_core))))
                out = block_forward(1, lo, end, x_t, mod_rows[l], others[-1][-1], b_rel[2:, l], *consts, (y, o, lse, h_t, z), False, n_tp * (end and l == n_l - 1))
                y, o, lse, z = out[:4]
            branch, x_cur = out[3:]
            saved.append((x_t, y, o, lse, h_t, branch))
            ws.append(others)
        d_late, tie = lax.optimization_barrier((d_out, tie))
        g_tok = swap(d_late.reshape(n_tp, n_b, s_own, dim))
        x_out = swap(x_cur)

        grads, small = [None] * n_l, [None] * n_l
        top = n_l - 1
        g_t, d_br, sums_in = edge(g_tok, (), (mod_rows[top], saved[top][5]), True, 0)
        d_gate, d_bias = sums_in[:, 0], sums_in[:, 1]
        for l in reversed(range(n_l)):
            x_t, y, o, lse, h_t, branch = saved[l]
            if l == 0:
                d_br, x_out = lax.optimization_barrier((d_br, x_out))
            d_hs, d_qk, gb, gw = [], 0.0, [], []
            for j, width, w_other in ws[l]:
                keep, send, gb_j, dqk_j, dh_j = block_backward(j, width, d_br, h_t, (*w_own[l], *w_other), qk[l], cos_t, sin_t, y, o, lse)
                d_hs.append(dh_j)
                d_qk = d_qk + dqk_j
                gb.append(gb_j)
                near = lax.ppermute(send, "tp", peer_core)
                leaving = (keep[1].astype(F32) + near[1].astype(F32)).astype(BF16)
                far = lax.ppermute(leaving, "tp", across)
                gw.append((keep[0].astype(F32) + near[0].astype(F32) + far.astype(F32)).astype(BF16))
            entry = (mod_rows[l - 1], saved[l - 1][5]) if l > 0 else ()
            edge_out = edge(g_t, (x_t, mod_rows[l], d_hs), entry, False, n_tp * (l == 0))
            g_t, sums = edge_out[0], edge_out[-1]
            grads[l] = jnp.concatenate(gw)
            d_mod = jnp.stack([sums[:, 0], sums[:, 1], d_gate], axis=1)
            gb = jnp.concatenate(gb, axis=2).reshape(2, 2, n_j * cols)
            gb = jnp.stack([lax.dynamic_index_in_dim(lax.dynamic_index_in_dim(gb, (i ^ me) % 2, 0, keepdims=False), (i ^ me) // 2, 0, keepdims=False) for i in range(n_tp)])
            small[l] = jnp.concatenate([d_mod.reshape(-1), jnp.sum(d_bias, axis=0), d_qk.reshape(-1), gb.reshape(-1)])
            if l > 0:
                d_br = edge_out[1]
                d_gate, d_bias = sums[:, 2], sums[:, 3]

        gathered = swap(jnp.broadcast_to(jnp.stack(small), (n_tp, n_l, small[0].shape[0])))
        grad_x = swap(g_t)
        n_mod = n_b * 3 * dim
        d_mod = jnp.moveaxis(gathered[:, :, :n_mod].reshape(n_tp, n_l, n_b, 3 * dim), 1, 0).reshape(n_l, n_all, 3 * dim)
        sums = jnp.sum(gathered[:, :, n_mod:], axis=0)
        g_wmod = wmod_grad(silu_all, d_mod)
        g_bmod = jnp.sum(d_mod, axis=1)
        g_qk = interleave(sums[:, dim:dim + 2 * e].reshape(n_l, 2, e), e)
        g_b = lax.dynamic_index_in_dim(sums[:, dim + 2 * e:].reshape(n_l, n_tp, n_j, cols), me, 1, keepdims=False)
        g_bin = jnp.concatenate([interleave(g_b[..., :e], e), interleave(g_b[..., e:2 * e], e), g_b[..., 2 * e:]], axis=-1)
        gw_all = jnp.stack(grads)
        g_win = jnp.einsum("ec,lhed->ldhc", perm_mat, gw_all[:, :, :cols], preferred_element_type=F32).astype(BF16)
        return (x_out.reshape(n_all, s_own, dim), grad_x.reshape(n_all, s_own, dim), g_wmod, g_bmod, g_win, g_bin, g_qk[:, 0], g_qk[:, 1], gw_all[:, :, cols:], sums[:, :dim])

    return jax.shard_map(device_step, mesh=mesh, in_specs=in_specs, out_specs=out_specs, check_vma=False)
```
